256 devices in a mesh: gx: 64 (over z_lo, x, y), gy: 4 (over z_hi, core).
Axes of the slice: x: 4, y: 4, z: 8 (z_hi: 2, z_lo: 4; z = z_hi * 4 + z_lo), core: 2. Of those that a mesh axis runs over, the one named last changes fastest.
Arguments:
- date_key: int32 [3145728], P(('gx', 'gy')), may hold values from 0 to 4095
- store_key: int32 [3145728], P(('gx', 'gy')), may hold values from 0 to 65535
- product_key: int32 [3145728], P(('gx', 'gy')), may hold values from 0 to 1048575
- revenue: bfloat16 [3145728], P(('gx', 'gy')), may hold values from -0.59765625 to 0.59765625
- row_counts: int32 [256], P(('gx', 'gy')), may hold values from 1 to 12288, 1966080 in all
- date_years: int32 [512], P('gx'), may hold values from -2147483648 to 2147483646
- date_flags: int32 [128], P('gx'), may hold values from -2147483648 to 2147483646
- store_flags: int32 [2048], P('gx'), may hold values from -2147483648 to 2147483646
- product_flags: int32 [32768], P('gx'), may hold values from -2147483648 to 2147483646
- brand_words: int32 [349696], P('gx'), may hold values from 0 to 1073741823
Outputs:
- revenue_groups: float32 [16, 1024], replicated
The draws below stay inside these ranges and needn't reach their ends.
Inputs may be any that keep to these rules, and one draw needn't show every extreme that they name: Rows d * 12288 to d * 12288 + row_counts[d] - 1 of the fact arrays are live; the largest count equals 12288. `date_years`: date k's year code is in bits 4 * (k % 8) of word k // 8. `date_flags`: bit k % 32 of word k // 32 is the flag of row k. `store_flags`: bit k % 32 of word k // 32 is the flag of row k. `product_flags`: bit k % 32 of word k // 32 is the flag of row k. `brand_words`: product with shard o and local index l holds its brand code in bits 10 * (l % 3) of word o * 5464 + l // 3; words past a shard's products are unused.
All inputs are finite; a program needn't handle non-finite values. No bound on the sum of `row_counts` on one device may be relied on, other than what follows from the above.
Results may differ from the reference program's by a relative error of at most 0.0003.
Values sent between devices are 32-bit elements; how exact they have to be, the bound alone decides.
No kernel may reach another device: no remote copies, remote signals or barrier semaphores. Data moves between devices by JAX's collectives and lax.ppermute only.
A program may use at most 64 MiB of HBM per device.

```python
import math
import jax
import jax.numpy as jnp
import numpy as np

DATES = 4096
STORES = 65536
PRODUCTS = 1048576
BRANDS = 1024
YEARS = 16
FACT_DEV = 12288
BW_DEV = 5464
N_GX = 64
N_GY = 4
DEVICES = 256


def touch_ends(drawn, rng, low, high):
    spot = [jax.random.randint(jax.random.fold_in(rng, axis), (), 0, length) for axis, length in enumerate(drawn.shape)]
    main_axis = drawn.shape.index(max(drawn.shape))
    neighbour = spot[:main_axis] + [(spot[main_axis] + 1) % drawn.shape[main_axis]] + spot[main_axis + 1:]
    return drawn.at[tuple(spot)].set(low).at[tuple(neighbour)].set(high)


def levels(stream_key, dims, shards, least, high):
    def one(axis_at, shards_of):
        draws = jax.random.uniform(jax.random.fold_in(jax.random.fold_in(stream_key, 6), axis_at), (shards_of,), jnp.float32, least / len(shards), high / len(shards))
        return jnp.repeat(jnp.exp(draws), dims[axis_at] // shards_of).reshape((-1,) + (1,) * (len(dims) - axis_at - 1))

    gain = one(*shards[0])
    for cut in shards[1:]:
        gain = gain * one(*cut)
    return gain


def wide_ids(stream_key, dims, count, skew):
    loads = [min(1 << octave, count + 1 - (1 << octave)) * (1 << 20) // math.isqrt((1 << octave) ** skew) + 1 for octave in range((count + 1).bit_length()) if 1 << octave <= count]
    width = 1 + sum(loads) // (1 << 30)
    table = np.cumsum(np.array([max(1, weight // width) for weight in loads]))
    ticket = jax.random.randint(jax.random.fold_in(stream_key, 1), dims, 0, int(table[len(loads) - 1]))
    start = jnp.left_shift(1, jnp.searchsorted(jnp.asarray(table, jnp.int32), ticket, side="right").astype(jnp.int32))
    standing = start - 1 + jax.random.randint(jax.random.fold_in(stream_key, 4), dims, 0, 1 << 30) % jnp.minimum(start, count + 1 - start)
    return jax.random.permutation(jax.random.fold_in(stream_key, 2), count)[standing].astype(jnp.int32)


def length_profile(number_of, total, most, lean):
    weights = [(1 << 20) // math.isqrt(standing ** lean) + 1 for standing in range(2, number_of + 1)]
    spare, counts = total - most - (number_of - 1), [1] * (number_of - 1)
    while spare > 0:
        free = [i for i in range(number_of - 1) if counts[i] < most]
        pool, remaining = sum([weights[i] for i in free]), spare
        for i in free:
            extra = min(most - counts[i], max(1, remaining * weights[i] // pool), spare)
            counts[i] = counts[i] + extra
            spare = spare - extra
    return np.array([most] + counts)


def uneven_parts(own_key, count, total, most, slope):
    if count == 2:
        one = jax.random.randint(own_key, (), max(1, total - most), min(most, total - 1) + 1)
        return jnp.stack([one, total - one])
    lengths = jnp.asarray(length_profile(count, total, most, slope), jnp.int32)
    couples = (count - 1) // 2
    giver, sink = lengths[1:1 + 2 * couples:2], lengths[2:2 + 2 * couples:2]
    slack = jnp.minimum(giver - 1, most - sink)
    moved = jax.random.randint(jax.random.fold_in(own_key, 1), (couples,), 0, 1 << 20) % (slack + 1)
    lengths = lengths.at[1:1 + 2 * couples:2].set(giver - moved).at[2:2 + 2 * couples:2].set(sink + moved)
    return lengths[jax.random.permutation(jax.random.fold_in(own_key, 2), count)]


def normal_values(rng, extent, spread, most, pieces=(), kind=jnp.bfloat16):
    loudness = levels(rng, extent, pieces, -0.22, 0.18) if pieces else 1.0
    drawn = jax.random.normal(rng, extent, jnp.float32) * spread * loudness
    return jnp.minimum(jnp.maximum(drawn, -most), most).astype(kind)


def setup_inputs(seed: int = 0) -> dict:
    streams_of = jax.random.split(jax.random.key(seed), 11)
    date_key = touch_ends(jax.random.randint(streams_of[0], (FACT_DEV * DEVICES,), 0, DATES), jax.random.fold_in(streams_of[0], 1), 0, DATES - 1).astype(jnp.int32)
    store_key = touch_ends(jax.random.randint(streams_of[1], (FACT_DEV * DEVICES,), 0, STORES), jax.random.fold_in(streams_of[1], 1), 0, STORES - 1).astype(jnp.int32)
    product_key = touch_ends(wide_ids(streams_of[2], (FACT_DEV * DEVICES,), PRODUCTS, 1), jax.random.fold_in(streams_of[2], 3), 0, PRODUCTS - 1).astype(jnp.int32)
    revenue = normal_values(streams_of[3], (FACT_DEV * DEVICES,), 0.1, 0.59765625, ((0, 256),))
    row_counts = uneven_parts(streams_of[4], DEVICES, DEVICES * FACT_DEV * 5 // 8, FACT_DEV, 2).astype(jnp.int32)
    date_years = touch_ends(jax.random.randint(streams_of[5], (DATES // 8,), -2147483648, 2147483647), jax.random.fold_in(streams_of[5], 1), -2147483648, 2147483646).astype(jnp.int32)
    date_flags = touch_ends(jax.random.randint(streams_of[6], (DATES // 32,), -2147483648, 2147483647), jax.random.fold_in(streams_of[6], 1), -2147483648, 2147483646).astype(jnp.int32)
    store_flags = touch_ends(jax.random.randint(streams_of[7], (STORES // 32,), -2147483648, 2147483647), jax.random.fold_in(streams_of[7], 1), -2147483648, 2147483646).astype(jnp.int32)
    product_flags = touch_ends(jax.random.randint(streams_of[8], (PRODUCTS // 32,), -2147483648, 2147483647), jax.random.fold_in(streams_of[8], 1), -2147483648, 2147483646).astype(jnp.int32)
    brand_words = touch_ends(jax.random.randint(streams_of[9], (BW_DEV * N_GX,), 0, 1073741824), jax.random.fold_in(streams_of[9], 1), 0, 1073741823).astype(jnp.int32)
    return dict(date_key=date_key, store_key=store_key, product_key=product_key, revenue=revenue, row_counts=row_counts, date_years=date_years, date_flags=date_flags, store_flags=store_flags, product_flags=product_flags, brand_words=brand_words)


def pick_bits(packed, position, width_bits):
    per_word = 32 // width_bits
    chosen = packed[position // per_word]
    shifted = jnp.right_shift(chosen, (position % per_word) * width_bits)
    return jnp.bitwise_and(shifted, (1 << width_bits) - 1)


def reference(date_key, store_key, product_key, revenue, row_counts, date_years, date_flags, store_flags, product_flags, brand_words):
    prod_shard = PRODUCTS // N_GX
    positions = jnp.arange(FACT_DEV * N_GX * N_GY, dtype=jnp.int32)
    live_rows = (positions % FACT_DEV) < row_counts[positions // FACT_DEV]
    year_code = pick_bits(date_years, date_key, 4)
    passed = pick_bits(date_flags, date_key, 1) * pick_bits(store_flags, store_key, 1) * pick_bits(product_flags, product_key, 1)
    owner_idx = product_key // prod_shard
    local_idx = product_key % prod_shard
    word_val = brand_words[owner_idx * BW_DEV + local_idx // 3]
    brand_code = jnp.bitwise_and(jnp.right_shift(word_val, (local_idx % 3) * 10), 1023)
    kept_rows = live_rows & (passed == 1)
    amount = jnp.where(kept_rows, revenue.astype(jnp.float32), jnp.float32(0))
    group_id = year_code * BRANDS + brand_code
    totals = jax.ops.segment_sum(amount, group_id, num_segments=YEARS * BRANDS)
    return totals.reshape(YEARS, BRANDS)
```

```python
import functools

import jax
import jax.numpy as jnp
from jax import lax
from jax.experimental import pallas as pl
from jax.experimental.pallas import tpu as pltpu
from jax.sharding import PartitionSpec as P

BRANDS = 1024
YEARS = 16
AXES = ("gx", "gy")
LANES = 128
BRAND_ROWS = 22
FLAG_ROWS = 2
BLOCK_ROWS = BRAND_ROWS + FLAG_ROWS
OWNERS = 64


def place_of(index):
    gx, gy = index // 4, index % 4
    return dict(zl=gx // 16, x=gx // 4 % 4, y=gx % 4, zh=gy // 2, c=gy % 2)


def index_of(place):
    gx = place["zl"] * 16 + place["x"] * 4 + place["y"]
    return gx * 4 + place["zh"] * 2 + place["c"]


def shifted(value, **steps):
    sizes = dict(zl=4, x=4, y=4, zh=2, c=2)
    pairs = []
    for source in range(256):
        place = place_of(source)
        if "z" in steps:
            z = (place["zh"] * 4 + place["zl"] + steps["z"]) % 8
            place["zh"], place["zl"] = z // 4, z % 4
        for axis, step in steps.items():
            if axis != "z":
                place[axis] = (place[axis] + step) % sizes[axis]
        pairs.append((source, index_of(place)))
    return lax.ppermute(value, AXES, pairs)


def lane_gather(rows, lanes):
    return jnp.take_along_axis(rows, lanes, axis=1, mode="promise_in_bounds")


def spread(ref, row):
    return jnp.broadcast_to(ref[pl.ds(row, 1), :], (8, LANES))


def pick(values, bits):
    for bit in bits:
        values = [
            values[i] if i + 1 == len(values) else jnp.where(bit, values[i + 1], values[i])
            for i in range(0, len(values), 2)
        ]
        if len(values) == 1:
            break
    return values[0]


def join_kernel(
    where_ref,
    date_ref,
    store_ref,
    product_ref,
    money_ref,
    *refs,
):
    tables, (out_ref, small_ref) = refs[:8], refs[8:]
    zl, x, y, c = (where_ref[i] for i in range(4))
    count = where_ref[4]
    lane = lax.broadcasted_iota(jnp.int32, (8, LANES), 1)
    sub = lax.broadcasted_iota(jnp.int32, (8, LANES), 0)

    small_ref[...] = jnp.zeros_like(small_ref)

    def owner_of(kx, row):
        ky, kz = row // 4, row % 4
        return ((zl - kz) & 3) * 16 + ((x - kx) & 3) * 4 + ((y - ky) & 3)

    for kx in range(4):
        for ky in range(4):
            for kz in range(4):
                at = (ky * 4 + kz) * BLOCK_ROWS + BRAND_ROWS - 1
                owner = owner_of(kx, ky * 4 + kz)
                mine = tables[kx][pl.ds(at, 1), :]
                other = tables[4 + kx][pl.ds(at, 1), :]
                line = jnp.broadcast_to(jnp.where(c == 1, mine, other), (8, LANES))
                lane_from = jnp.where(
                    sub == 0,
                    lane & 31,
                    jnp.where(sub == 1, 32 + (lane & 7), 40 + (lane & 1)),
                )
                moved = lane_gather(line, lane_from)
                stores = jnp.where((lane >> 5) == (owner & 3), moved, 0)[0:1]
                years = jnp.where((lane >> 3) == (owner & 15), moved, 0)[1:2]
                days = jnp.where((lane >> 1) == owner, moved, 0)[2:3]
                small_ref[pl.ds(owner // 4, 1), :] += stores
                small_ref[pl.ds(16 + owner // 16, 1), :] += years
                small_ref[pl.ds(20, 1), :] += days

    high_row = lax.broadcasted_iota(jnp.int32, (LANES, LANES), 0)
    out_ref[...] = jnp.zeros_like(out_ref)

    def add_block(block, _):
        at = pl.ds(pl.multiple_of(block * 8, 8), 8)
        date = date_ref[at, :]
        store = store_ref[at, :]
        product = product_ref[at, :]

        year_word = lane_gather(spread(small_ref, 16), (date >> 3) & 127)
        word_row = date >> 10
        for i in range(1, 4):
            year_word = jnp.where(
                word_row == i, lane_gather(spread(small_ref, 16 + i), (date >> 3) & 127), year_word
            )
        year = (year_word >> ((date & 7) * 4)) & 15
        day_bit = lane_gather(spread(small_ref, 20), date >> 5) >> (date & 31)
        store_lane, store_row = (store >> 5) & 127, store >> 12
        store_word = pick(
            [lane_gather(spread(small_ref, i), store_lane) for i in range(16)],
            [((store_row >> b) & 1) == 1 for b in range(4)],
        )
        passed = day_bit & (store_word >> (store & 31))

        owner = product >> 14
        local = product & 16383
        word = (local * 21846) >> 16
        digit = local - word * 3
        row, word_lane = word >> 7, word & 127
        half = (row >= BRAND_ROWS).astype(jnp.int32)
        row = row - half * BRAND_ROWS
        flag_row, flag_lane = local >> 12, (local >> 5) & 127
        key = owner * 2 + half
        flag_key = owner * 2 + (flag_row >> 1)
        row_bits = [((row >> b) & 1) == 1 for b in range(5)]
        flag_bits = [(flag_row & 1) == 1]

        def search(carry):
            for kx in range(4):
                for side in range(2):
                    table = tables[side * 4 + kx]
                    side_now = (c + side) & 1

                    def step(j, carry, table=table, kx=kx, side_now=side_now):
                        found, flags = carry
                        key_now = owner_of(kx, j) * 2 + side_now
                        start = j * BLOCK_ROWS
                        got = pick(
                            [
                                lane_gather(spread(table, start + i), word_lane)
                                for i in range(BRAND_ROWS)
                            ],
                            row_bits,
                        )
                        found = jnp.where(key == key_now, got, found)
                        got = pick(
                            [
                                lane_gather(spread(table, start + BRAND_ROWS + i), flag_lane)
                                for i in range(FLAG_ROWS)
                            ],
                            flag_bits,
                        )
                        flags = jnp.where(flag_key == key_now, got, flags)
                        return found, flags

                    carry = lax.fori_loop(0, 16, step, carry)
            return carry

        zero = jnp.zeros((8, LANES), jnp.int32)
        found, flags = search((zero, zero))
        brand = (found >> (digit * 10)) & 1023
        passed = passed & (flags >> (local & 31)) & 1
        place = block * 1024 + sub * LANES + lane
        keep = (passed == 1) & (place < count)
        amount = jnp.where(keep, money_ref[at, :].astype(jnp.float32), 0.0)
        high = (brand >> 7) * YEARS + year
        low = brand & 127
        weighted, low_hot = [], []
        for s in range(8):
            weighted.append(
                jnp.where(high_row == high[s : s + 1, :], amount[s : s + 1, :], 0.0).astype(
                    jnp.bfloat16
                )
            )
            low_hot.append((high_row == low[s : s + 1, :]).astype(jnp.float32).astype(jnp.bfloat16))
        out_ref[...] += lax.dot_general(
            jnp.concatenate(weighted, axis=1),
            jnp.concatenate(low_hot, axis=1),
            (((1,), (1,)), ((), ())),
            preferred_element_type=jnp.float32,
        )
        return 0

    lax.fori_loop(0, (count + 1023) // 1024, add_block, 0)


def joined(where, date, store, product, money, tables):
    vmem = pl.BlockSpec(memory_space=pltpu.VMEM)
    return pl.pallas_call(
        join_kernel,
        out_shape=jax.ShapeDtypeStruct((LANES, LANES), jnp.float32),
        in_specs=[pl.BlockSpec(memory_space=pltpu.SMEM)] + [vmem] * 12,
        out_specs=vmem,
        scratch_shapes=[pltpu.VMEM((24, LANES), jnp.int32)],
        cost_estimate=pl.CostEstimate(flops=10**8, bytes_accessed=10**6, transcendentals=0),
        compiler_params=pltpu.CompilerParams(vmem_limit_bytes=8 * 2**20),
    )(where, date, store, product, money, *tables)


def gather_tables(block):
    along_z = [block] + [shifted(block, zl=k) for k in range(1, 4)]
    line = jnp.concatenate(along_z, axis=0)
    along_y = [line] + [shifted(line, y=k) for k in range(1, 4)]
    plane = jnp.concatenate(along_y, axis=0)
    mine = [plane] + [shifted(plane, x=k) for k in range(1, 4)]
    other = [shifted(part, c=1) for part in mine]
    return mine + other


def sum_everywhere(partial, x, c):
    def part(dc, dx):
        at = ((c + dc) & 1) * 64 + ((x + dx) & 3) * 16
        return lax.dynamic_slice_in_dim(partial, at, 16, 0)

    got = {}
    for dc in range(2):
        for dx in range(4):
            piece = part(dc, dx)
            got[dc, dx] = shifted(piece, c=dc, x=dx) if dc or dx else piece
    sums = [got[0, dx] + got[1, dx] for dx in range(4)]
    total = (sums[0] + sums[2]) + (sums[1] + sums[3])
    by_y = [total] + [shifted(total, y=k) for k in range(1, 4)]
    total = (by_y[0] + by_y[2]) + (by_y[1] + by_y[3])
    by_z = [total] + [shifted(total, z=k) for k in range(1, 8)]
    pairs = [by_z[k] + by_z[k + 4] for k in range(4)]
    total = (pairs[0] + pairs[2]) + (pairs[1] + pairs[3])
    pieces = [
        shifted(total, c=dc, x=dx) if dc or dx else total for dc in range(2) for dx in range(4)
    ]
    return pl.pallas_call(
        lay_kernel,
        out_shape=jax.ShapeDtypeStruct((YEARS, BRANDS), jnp.float32),
        in_specs=[pl.BlockSpec(memory_space=pltpu.SMEM)]
        + [pl.BlockSpec(memory_space=pltpu.VMEM)] * 8,
        out_specs=pl.BlockSpec(memory_space=pltpu.VMEM),
        compiler_params=pltpu.CompilerParams(vmem_limit_bytes=2**20),
    )(jnp.stack([x, c]), *pieces)


def lay_kernel(where_ref, *refs):
    pieces, out_ref = refs[:8], refs[8]
    for dc in range(2):
        for dx in range(4):
            at = ((where_ref[1] - dc) & 1) * 4 + ((where_ref[0] - dx) & 3)
            out_ref[:, pl.ds(pl.multiple_of(at * LANES, LANES), LANES)] = pieces[dc * 4 + dx][...]


def shards(
    date_key,
    store_key,
    product_key,
    revenue,
    row_counts,
    date_years,
    date_flags,
    store_flags,
    product_flags,
    brand_words,
):
    gx, gy = lax.axis_index("gx"), lax.axis_index("gy")
    zl, x, y, c = gx // 16, gx // 4 % 4, gx % 4, gy % 2
    split = BRAND_ROWS * LANES
    low = jnp.concatenate([brand_words[:split], product_flags[:256]])
    pad = jnp.zeros(2 * split - LANES - brand_words.shape[0], jnp.int32)
    small_pad = jnp.zeros(LANES - 42, jnp.int32)
    high = jnp.concatenate(
        [
            brand_words[split:],
            pad,
            store_flags,
            date_years,
            date_flags,
            small_pad,
            product_flags[256:],
        ]
    )
    block = jnp.where(c == 0, low, high).reshape(BLOCK_ROWS, LANES)
    tables = gather_tables(block)
    where = jnp.stack([zl, x, y, c, row_counts[0]])
    facts = [a.reshape(-1, LANES) for a in (date_key, store_key, product_key, revenue)]
    partial = joined(where, *facts, tables)
    return sum_everywhere(partial, x, c)


def solution(mesh):
    placed = (P(AXES),) * 5 + (P("gx"),) * 5
    return jax.shard_map(shards, mesh=mesh, in_specs=placed, out_specs=P(), check_vma=False)
```

```python
import functools

import jax
import jax.numpy as jnp
from jax import lax
from jax.experimental import pallas as pl
from jax.experimental.pallas import tpu as pltpu
from jax.sharding import PartitionSpec as P

BRANDS = 1024
YEARS = 16
AXES = ("gx", "gy")
LANES = 128
BRAND_ROWS = 22
FLAG_ROWS = 2
BLOCK_ROWS = BRAND_ROWS + FLAG_ROWS
UNROLL = 4


def place_of(index):
    gx, gy = index // 4, index % 4
    return dict(zl=gx // 16, x=gx // 4 % 4, y=gx % 4, zh=gy // 2, c=gy % 2)


def index_of(place):
    gx = place["zl"] * 16 + place["x"] * 4 + place["y"]
    return gx * 4 + place["zh"] * 2 + place["c"]


def shifted(value, **steps):
    sizes = dict(zl=4, x=4, y=4, zh=2, c=2)
    pairs = []
    for source in range(256):
        place = place_of(source)
        if "z" in steps:
            z = (place["zh"] * 4 + place["zl"] + steps["z"]) % 8
            place["zh"], place["zl"] = z // 4, z % 4
        for axis, step in steps.items():
            if axis != "z":
                place[axis] = (place[axis] + step) % sizes[axis]
        pairs.append((source, index_of(place)))
    return lax.ppermute(value, AXES, pairs)


def lane_gather(rows, lanes):
    return jnp.take_along_axis(rows, lanes, axis=1, mode="promise_in_bounds")


def spread(ref, row):
    return jnp.broadcast_to(ref[pl.ds(row, 1), :], (8, LANES))


def join_kernel(
    where_ref,
    date_ref,
    store_ref,
    product_ref,
    money_ref,
    *refs,
):
    tables, out_ref, (small_ref, keep_ref, meta_ref, money_scratch) = refs[:8], refs[8], refs[9:]
    zl, x, y, c = (where_ref[i] for i in range(4))
    count = where_ref[4]
    lane = lax.broadcasted_iota(jnp.int32, (8, LANES), 1)
    sub = lax.broadcasted_iota(jnp.int32, (8, LANES), 0)
    rows = date_ref.shape[0]

    def owner_of(kx, row):
        ky, kz = row >> 2, row & 3
        return ((zl - kz) & 3) * 16 + ((x - kx) & 3) * 4 + ((y - ky) & 3)

    small_ref[...] = jnp.zeros_like(small_ref)
    lane_from = jnp.where(
        sub == 0, lane & 31, jnp.where(sub == 1, 32 + (lane & 7), 40 + (lane & 1))
    )
    for kx in range(4):
        for row in range(16):
            at = row * BLOCK_ROWS + BRAND_ROWS - 1
            owner = owner_of(kx, row)
            mine = tables[kx][pl.ds(at, 1), :]
            other = tables[4 + kx][pl.ds(at, 1), :]
            line = jnp.broadcast_to(jnp.where(c == 1, mine, other), (8, LANES))
            moved = lane_gather(line, lane_from)
            stores = jnp.where((lane >> 5) == (owner & 3), moved, 0)[0:1]
            years = jnp.where((lane >> 3) == (owner & 15), moved, 0)[1:2]
            days = jnp.where((lane >> 1) == owner, moved, 0)[2:3]
            small_ref[pl.ds(owner >> 2, 1), :] += stores
            small_ref[pl.ds(16 + (owner >> 4), 1), :] += years
            small_ref[pl.ds(20, 1), :] += days

    keep_ref[...] = jnp.zeros_like(keep_ref)
    meta_ref[...] = jnp.zeros_like(meta_ref)

    def filter_block(block, _):
        at = pl.ds(pl.multiple_of(block * 8, 8), 8)
        date, store, product = date_ref[at, :], store_ref[at, :], product_ref[at, :]
        year_lane, year_row = (date >> 3) & 127, date >> 10
        year_word = jnp.zeros_like(date)
        for i in range(4):
            year_word = jnp.where(
                year_row == i, lane_gather(spread(small_ref, 16 + i), year_lane), year_word
            )
        year = (year_word >> ((date & 7) * 4)) & 15
        passed = lane_gather(spread(small_ref, 20), date >> 5) >> (date & 31)
        store_lane, store_row = (store >> 5) & 127, store >> 12
        store_word = jnp.zeros_like(store)
        for i in range(16):
            store_word = jnp.where(
                store_row == i, lane_gather(spread(small_ref, i), store_lane), store_word
            )
        passed &= store_word >> (store & 31)

        owner = product >> 14
        flag_row, flag_lane = (product >> 12) & 3, (product >> 5) & 127
        flag_key = owner * 2 + (flag_row >> 1)
        flag_row &= 1

        def step(turn, flags):
            flags = list(flags)
            for kx in range(4):
                for side in range(2):
                    table = tables[side * 4 + kx]
                    for u in range(8):
                        start = turn * (8 * BLOCK_ROWS)
                        key_now = owner_of(kx, turn * 8 + u) * 2 + ((c + side) & 1)
                        row = jnp.where(flag_key == key_now, flag_row, -1)
                        for i in range(FLAG_ROWS):
                            got = lane_gather(
                                spread(table, start + (u * BLOCK_ROWS + BRAND_ROWS + i)), flag_lane
                            )
                            flags[kx] = jnp.where(row == i, got, flags[kx])
            return tuple(flags)

        flags = lax.fori_loop(0, 2, step, (jnp.zeros_like(date),) * 4)
        passed &= (flags[0] | flags[1] | flags[2] | flags[3]) >> (product & 31)
        place = block * (8 * LANES) + sub * LANES + lane
        passed &= (place < count).astype(jnp.int32)
        keep_ref[at, :] = passed & 1
        meta_ref[at, :] = product | (year << 20)
        return 0

    lax.fori_loop(0, (count + 1023) // 1024, filter_block, 0)

    keep = keep_ref[...]
    above = lax.broadcasted_iota(jnp.int32, (LANES, rows), 0) > lax.broadcasted_iota(
        jnp.int32, (LANES, rows), 1
    )
    dropped = lax.dot_general(
        jnp.where(above, 1.0, 0.0).astype(jnp.bfloat16),
        (1 - keep).astype(jnp.float32).astype(jnp.bfloat16),
        (((1,), (0,)), ((), ())),
        preferred_element_type=jnp.float32,
    )[:rows].astype(jnp.int32)
    valid = jnp.int32(-(2**31))
    meta = jnp.where(keep == 1, meta_ref[...] | (dropped << 24) | valid, 0)
    money = money_ref[...].astype(jnp.float32)
    for b in range(7):
        bit = jnp.int32(1 << (24 + b))
        coming = pltpu.roll(meta, rows - (1 << b), 0)
        coming_money = pltpu.roll(money, rows - (1 << b), 0)
        take = (coming & bit) != 0
        meta = jnp.where(take, coming, jnp.where((meta & bit) != 0, 0, meta))
        money = jnp.where(take, coming_money, money)
    meta_ref[...] = meta
    money_scratch[...] = money
    deepest = jnp.max(jnp.sum(keep, axis=0, keepdims=True))

    high_row = lax.broadcasted_iota(jnp.int32, (LANES, LANES), 0)
    out_ref[...] = jnp.zeros_like(out_ref)

    def add_block(block, _):
        at = pl.ds(pl.multiple_of(block * 8, 8), 8)
        meta = meta_ref[at, :]
        product, year = meta & 0xFFFFF, (meta >> 20) & 15
        local = product & 16383
        word = (local * 21846) >> 16
        digit = local - word * 3
        row, word_lane = word >> 7, word & 127
        half = (row >= BRAND_ROWS).astype(jnp.int32)
        row -= half * BRAND_ROWS
        key = (product >> 14) * 2 + half

        def step(turn, found):
            found = list(found)
            for u in range(UNROLL):
                for kx in range(4):
                    for side in range(2):
                        table = tables[side * 4 + kx]
                        start = turn * (UNROLL * BLOCK_ROWS)
                        key_now = owner_of(kx, turn * UNROLL + u) * 2 + ((c + side) & 1)
                        row_now = jnp.where(key == key_now, row, -1)
                        for i in range(BRAND_ROWS):
                            got = lane_gather(
                                spread(table, start + (u * BLOCK_ROWS + i)), word_lane
                            )
                            at = i % 4
                            found[at] = jnp.where(row_now == i, got, found[at])
            return tuple(found)

        found = lax.fori_loop(0, 16 // UNROLL, step, (jnp.zeros_like(meta),) * 4)
        found = found[0] | found[1] | found[2] | found[3]
        brand = (found >> (digit * 10)) & 1023
        amount = jnp.where(meta < 0, money_scratch[at, :], 0.0)
        high = (brand >> 7) * YEARS + year
        low = brand & 127
        weighted, low_hot = [], []
        for s in range(8):
            weighted.append(
                jnp.where(high_row == high[s : s + 1, :], amount[s : s + 1, :], 0.0).astype(
                    jnp.bfloat16
                )
            )
            low_hot.append((high_row == low[s : s + 1, :]).astype(jnp.float32).astype(jnp.bfloat16))
        out_ref[...] += lax.dot_general(
            jnp.concatenate(weighted, axis=1),
            jnp.concatenate(low_hot, axis=1),
            (((1,), (1,)), ((), ())),
            preferred_element_type=jnp.float32,
        )
        return 0

    lax.fori_loop(0, (deepest + 7) // 8, add_block, 0)


def joined(where, date, store, product, money, tables):
    vmem = pl.BlockSpec(memory_space=pltpu.VMEM)
    rows = date.shape[0]
    return pl.pallas_call(
        join_kernel,
        out_shape=jax.ShapeDtypeStruct((LANES, LANES), jnp.float32),
        in_specs=[pl.BlockSpec(memory_space=pltpu.SMEM)] + [vmem] * 12,
        out_specs=vmem,
        scratch_shapes=[
            pltpu.VMEM((24, LANES), jnp.int32),
            pltpu.VMEM((rows, LANES), jnp.int32),
            pltpu.VMEM((rows, LANES), jnp.int32),
            pltpu.VMEM((rows, LANES), jnp.float32),
        ],
        cost_estimate=pl.CostEstimate(flops=10**8, bytes_accessed=10**6, transcendentals=0),
        compiler_params=pltpu.CompilerParams(vmem_limit_bytes=8 * 2**20),
    )(where, date, store, product, money, *tables)


def gather_tables(block):
    along_z = [block] + [shifted(block, zl=k) for k in range(1, 4)]
    line = jnp.concatenate(along_z, axis=0)
    along_y = [line] + [shifted(line, y=k) for k in range(1, 4)]
    plane = jnp.concatenate(along_y, axis=0)
    mine = [plane] + [shifted(plane, x=k) for k in range(1, 4)]
    other = [shifted(part, c=1) for part in mine]
    return mine + other


def four(value):
    return (value[0] + value[2]) + (value[1] + value[3])


def sum_everywhere(partial, x, c):
    def half(at):
        return lax.dynamic_slice_in_dim(partial, at * 64, 64, 0)

    mine = half(c) + shifted(half(1 - c), c=1)

    def part(dx):
        return lax.dynamic_slice_in_dim(mine, ((x + dx) & 3) * 16, 16, 0)

    total = four([part(0)] + [shifted(part(k), x=k) for k in range(1, 4)])
    total = four([total] + [shifted(total, y=k) for k in range(1, 4)])
    total = four([total] + [shifted(total, zl=k) for k in range(1, 4)])
    total = total + shifted(total, zh=1)
    along = jnp.concatenate([total] + [shifted(total, x=k) for k in range(1, 4)], axis=0)
    pieces = [along, shifted(along, c=1)]
    return pl.pallas_call(
        lay_kernel,
        out_shape=jax.ShapeDtypeStruct((YEARS, BRANDS), jnp.float32),
        in_specs=[pl.BlockSpec(memory_space=pltpu.SMEM)]
        + [pl.BlockSpec(memory_space=pltpu.VMEM)] * 2,
        out_specs=pl.BlockSpec(memory_space=pltpu.VMEM),
        compiler_params=pltpu.CompilerParams(vmem_limit_bytes=2**20),
    )(jnp.stack([x, c]), *pieces)


def lay_kernel(where_ref, mine_ref, other_ref, out_ref):
    for dc, ref in enumerate((mine_ref, other_ref)):
        for dx in range(4):
            at = ((where_ref[1] - dc) & 1) * 4 + ((where_ref[0] - dx) & 3)
            out_ref[:, pl.ds(pl.multiple_of(at * LANES, LANES), LANES)] = ref[
                pl.ds(dx * 16, 16), :
            ]


def shards(
    date_key,
    store_key,
    product_key,
    revenue,
    row_counts,
    date_years,
    date_flags,
    store_flags,
    product_flags,
    brand_words,
):
    gx, gy = lax.axis_index("gx"), lax.axis_index("gy")
    zl, x, y, c = gx // 16, gx // 4 % 4, gx % 4, gy % 2
    split = BRAND_ROWS * LANES
    low = jnp.concatenate([brand_words[:split], product_flags[:256]])
    pad = jnp.zeros(2 * split - LANES - brand_words.shape[0], jnp.int32)
    small_pad = jnp.zeros(LANES - 42, jnp.int32)
    high = jnp.concatenate(
        [
            brand_words[split:],
            pad,
            store_flags,
            date_years,
            date_flags,
            small_pad,
            product_flags[256:],
        ]
    )
    block = jnp.where(c == 0, low, high).reshape(BLOCK_ROWS, LANES)
    tables = gather_tables(block)
    where = jnp.stack([zl, x, y, c, row_counts[0]])
    facts = [a.reshape(-1, LANES) for a in (date_key, store_key, product_key, revenue)]
    partial = joined(where, *facts, tables)
    return sum_everywhere(partial, x, c)


def solution(mesh):
    placed = (P(AXES),) * 5 + (P("gx"),) * 5
    return jax.shard_map(shards, mesh=mesh, in_specs=placed, out_specs=P(), check_vma=False)
```

```python
import functools

import jax
import jax.numpy as jnp
from jax import lax
from jax.experimental import pallas as pl
from jax.experimental.pallas import tpu as pltpu
from jax.sharding import PartitionSpec as P

BRANDS = 1024
YEARS = 16
AXES = ("gx", "gy")
LANES = 128
BRAND_ROWS = 22
FLAG_ROWS = 2
BLOCK_ROWS = BRAND_ROWS + FLAG_ROWS


def place_of(index):
    gx, gy = index // 4, index % 4
    return dict(zl=gx // 16, x=gx // 4 % 4, y=gx % 4, zh=gy // 2, c=gy % 2)


def index_of(place):
    gx = place["zl"] * 16 + place["x"] * 4 + place["y"]
    return gx * 4 + place["zh"] * 2 + place["c"]


def moved_by(value, move):
    pairs = []
    for source in range(256):
        place = place_of(source)
        move(place)
        pairs.append((source, index_of(place)))
    return lax.ppermute(value, AXES, pairs)


def shifted(value, **steps):
    sizes = dict(zl=4, x=4, y=4, zh=2, c=2)

    def move(place):
        for axis, step in steps.items():
            place[axis] = (place[axis] + step) % sizes[axis]

    return moved_by(value, move)


def mirrored(value):
    def move(place):
        place["zh"], place["zl"] = 1 - place["zh"], 3 - place["zl"]

    return moved_by(value, move)


def lane_gather(rows, lanes):
    return jnp.take_along_axis(rows, lanes, axis=1, mode="promise_in_bounds")


def spread(ref, row):
    return jnp.broadcast_to(ref[pl.ds(row, 1), :], (8, LANES))


def packed_up(keep, meta, money):
    rows = keep.shape[0]
    above = lax.broadcasted_iota(jnp.int32, (LANES, rows), 0) > lax.broadcasted_iota(
        jnp.int32, (LANES, rows), 1
    )
    dropped = lax.dot_general(
        jnp.where(above, 1.0, 0.0).astype(jnp.bfloat16),
        (1 - keep).astype(jnp.float32).astype(jnp.bfloat16),
        (((1,), (0,)), ((), ())),
        preferred_element_type=jnp.float32,
    )[:rows].astype(jnp.int32)
    meta = jnp.where(keep == 1, meta | (dropped << 24) | jnp.int32(-(2**31)), 0)
    for b in range(7):
        bit = jnp.int32(1 << (24 + b))
        coming = pltpu.roll(meta, rows - (1 << b), 0)
        coming_money = pltpu.roll(money, rows - (1 << b), 0)
        take = (coming & bit) != 0
        meta = jnp.where(take, coming, jnp.where((meta & bit) != 0, 0, meta))
        money = jnp.where(take, coming_money, money)
    return meta, money


def deepest(keep):
    return jnp.max(jnp.sum(keep, axis=0, keepdims=True))


def join_kernel(
    where_ref,
    date_ref,
    store_ref,
    product_ref,
    money_ref,
    *refs,
):
    tables, out_ref, (small_ref, keep_ref, meta_ref, money_scratch) = refs[:8], refs[8], refs[9:]
    zl, x, y, c = (where_ref[i] for i in range(4))
    count = where_ref[4]
    lane = lax.broadcasted_iota(jnp.int32, (8, LANES), 1)
    sub = lax.broadcasted_iota(jnp.int32, (8, LANES), 0)

    lane_from = jnp.where(
        sub == 0, lane & 31, jnp.where(sub == 1, 32 + (lane & 7), 40 + (lane & 1))
    )
    days = jnp.zeros((8, LANES), jnp.int32)
    for kz in range(4):
        oz = (zl - kz) & 3
        years = jnp.zeros((8, LANES), jnp.int32)
        for kx in range(4):
            ox = (x - kx) & 3
            stores = jnp.zeros((8, LANES), jnp.int32)
            for ky in range(4):
                oy = (y - ky) & 3
                at = (ky * 4 + kz) * BLOCK_ROWS + BRAND_ROWS - 1
                mine = tables[kx][pl.ds(at, 1), :]
                other = tables[4 + kx][pl.ds(at, 1), :]
                line = jnp.broadcast_to(jnp.where(c == 1, mine, other), (8, LANES))
                moved = lane_gather(line, lane_from)
                stores += jnp.where((lane >> 5) == oy, moved, 0)
                years += jnp.where((lane >> 3) == ox * 4 + oy, moved, 0)
                days += jnp.where((lane >> 1) == oz * 16 + ox * 4 + oy, moved, 0)
            small_ref[pl.ds(oz * 4 + ox, 1), :] = stores[0:1]
        small_ref[pl.ds(16 + oz, 1), :] = years[1:2]
    small_ref[pl.ds(20, 1), :] = days[2:3]

    keep_ref[...] = jnp.zeros_like(keep_ref)
    meta_ref[...] = jnp.zeros_like(meta_ref)

    def filter_block(first):
        at = pl.ds(pl.multiple_of(first, 8), 8)
        date, store = date_ref[at, :], store_ref[at, :]
        year_lane, year_row = (date >> 3) & 127, date >> 10
        year_word = jnp.zeros_like(date)
        for i in range(4):
            year_word = jnp.where(
                year_row == i, lane_gather(spread(small_ref, 16 + i), year_lane), year_word
            )
        year = (year_word >> ((date & 7) * 4)) & 15
        passed = lane_gather(spread(small_ref, 20), date >> 5) >> (date & 31)
        store_lane, store_row = (store >> 5) & 127, store >> 12
        store_word = jnp.zeros_like(store)
        for i in range(16):
            store_word = jnp.where(
                store_row == i, lane_gather(spread(small_ref, i), store_lane), store_word
            )
        passed &= store_word >> (store & 31)
        place = (first + sub) * LANES + lane
        passed &= (place < count).astype(jnp.int32)
        keep_ref[at, :] = passed & 1
        meta_ref[at, :] = product_ref[at, :] | (year << 20)

    def filter_blocks(turn, _):
        for u in range(4):
            filter_block(turn * 32 + u * 8)
        return 0

    lax.fori_loop(0, (count + 4095) // 4096, filter_blocks, 0)
    keep = keep_ref[...]
    meta, money = packed_up(keep, meta_ref[...], money_ref[...].astype(jnp.float32))
    meta_ref[...] = meta
    money_scratch[...] = money
    left = deepest(keep)
    keep_ref[...] = jnp.zeros_like(keep_ref)

    def search(rows_of, code, lanes, first, number, unroll):
        def step(turn, found):
            found = [list(f) for f in found]
            start = turn * (unroll * BLOCK_ROWS)
            code_now = [v - turn * (unroll * 256) for v in code]
            for u in range(unroll):
                for t in range(8):
                    for i in range(number):
                        row = spread(tables[t], start + (u * BLOCK_ROWS + first + i))
                        for q in range(rows_of):
                            at = i % 2
                            got = lane_gather(row, lanes[q])
                            found[q][at] = jnp.where(
                                code_now[q] == u * 256 + t * 32 + i, got, found[q][at]
                            )
            return tuple(tuple(f) for f in found)

        zero = jnp.zeros((8, LANES), jnp.int32)
        found = lax.fori_loop(0, 16 // unroll, step, ((zero, zero),) * rows_of)
        return [f[0] | f[1] for f in found]

    def code_of(product, half, row):
        oz, ox, oy = product >> 18, (product >> 16) & 3, (product >> 14) & 3
        table = (half ^ c) * 4 + ((x - ox) & 3)
        return (((y - oy) & 3) * 4 + ((zl - oz) & 3)) * 256 + table * 32 + row

    def product_blocks(turn, _):
        ats = [pl.ds(pl.multiple_of(turn * 16 + u * 8, 8), 8) for u in range(2)]
        metas = [meta_ref[at, :] for at in ats]
        products = [meta & 0xFFFFF for meta in metas]
        words = search(
            2,
            [code_of(p, (p >> 13) & 1, (p >> 12) & 1) for p in products],
            [(p >> 5) & 127 for p in products],
            BRAND_ROWS,
            FLAG_ROWS,
            8,
        )
        for at, meta, product, word in zip(ats, metas, products, words):
            keep_ref[at, :] = jnp.where(meta < 0, (word >> (product & 31)) & 1, 0)
        return 0

    lax.fori_loop(0, (left + 15) // 16, product_blocks, 0)
    keep = keep_ref[...]
    meta, money = packed_up(keep, meta_ref[...] & 0xFFFFFF, money_scratch[...])
    meta_ref[...] = meta
    money_scratch[...] = money
    left = deepest(keep)

    high_row = lax.broadcasted_iota(jnp.int32, (LANES, LANES), 0)
    out_ref[...] = jnp.zeros_like(out_ref)

    def add_block(block, _):
        at = pl.ds(pl.multiple_of(block * 8, 8), 8)
        meta = meta_ref[at, :]
        product, year = meta & 0xFFFFF, (meta >> 20) & 15
        local = product & 16383
        word = (local * 21846) >> 16
        digit = local - word * 3
        row, word_lane = word >> 7, word & 127
        half = (row >= BRAND_ROWS).astype(jnp.int32)
        code = code_of(product, half, row - half * BRAND_ROWS)
        (found,) = search(1, [code], [word_lane], 0, BRAND_ROWS, 4)
        brand = (found >> (digit * 10)) & 1023
        amount = jnp.where(meta < 0, money_scratch[at, :], 0.0)
        high = (brand >> 7) * YEARS + year
        low = brand & 127
        weighted, low_hot = [], []
        for s in range(8):
            weighted.append(
                jnp.where(high_row == high[s : s + 1, :], amount[s : s + 1, :], 0.0).astype(
                    jnp.bfloat16
                )
            )
            low_hot.append((high_row == low[s : s + 1, :]).astype(jnp.float32).astype(jnp.bfloat16))
        out_ref[...] += lax.dot_general(
            jnp.concatenate(weighted, axis=1),
            jnp.concatenate(low_hot, axis=1),
            (((1,), (1,)), ((), ())),
            preferred_element_type=jnp.float32,
        )
        return 0

    lax.fori_loop(0, (left + 7) // 8, add_block, 0)


def joined(where, date, store, product, money, tables):
    vmem = pl.BlockSpec(memory_space=pltpu.VMEM)
    rows = date.shape[0]
    return pl.pallas_call(
        join_kernel,
        out_shape=jax.ShapeDtypeStruct((LANES, LANES), jnp.float32),
        in_specs=[pl.BlockSpec(memory_space=pltpu.SMEM)] + [vmem] * 12,
        out_specs=vmem,
        scratch_shapes=[
            pltpu.VMEM((24, LANES), jnp.int32),
            pltpu.VMEM((rows, LANES), jnp.int32),
            pltpu.VMEM((rows, LANES), jnp.int32),
            pltpu.VMEM((rows, LANES), jnp.float32),
        ],
        cost_estimate=pl.CostEstimate(flops=10**8, bytes_accessed=10**6, transcendentals=0),
        compiler_params=pltpu.CompilerParams(vmem_limit_bytes=8 * 2**20),
    )(where, date, store, product, money, *tables)


def gather_tables(block):
    along_z = [block] + [shifted(block, zl=k) for k in range(1, 4)]
    line = jnp.concatenate(along_z, axis=0)
    along_y = [line] + [shifted(line, y=k) for k in range(1, 4)]
    plane = jnp.concatenate(along_y, axis=0)
    mine = [plane] + [shifted(plane, x=k) for k in range(1, 4)]
    other = [shifted(part, c=1) for part in mine]
    return mine + other


def four(value):
    return (value[0] + value[2]) + (value[1] + value[3])


def sum_everywhere(partial, c):
    def half(at):
        return lax.dynamic_slice_in_dim(partial, at * 64, 64, 0)

    total = half(c) + shifted(half(1 - c), c=1)
    total = four([total] + [shifted(total, x=k) for k in range(1, 4)])
    total = four([total] + [shifted(total, y=k) for k in range(1, 4)])
    total = four([total] + [shifted(total, zl=k) for k in range(1, 4)])
    total = total + mirrored(total)
    return pl.pallas_call(
        lay_kernel,
        out_shape=jax.ShapeDtypeStruct((YEARS, BRANDS), jnp.float32),
        in_specs=[pl.BlockSpec(memory_space=pltpu.SMEM)]
        + [pl.BlockSpec(memory_space=pltpu.VMEM)] * 2,
        out_specs=pl.BlockSpec(memory_space=pltpu.VMEM),
        compiler_params=pltpu.CompilerParams(vmem_limit_bytes=2**20),
    )(c[None], total, shifted(total, c=1))


def lay_kernel(c_ref, mine_ref, other_ref, out_ref):
    for side, ref in enumerate((mine_ref, other_ref)):
        for i in range(4):
            at = (c_ref[0] ^ side) * 4 + i
            out_ref[:, pl.ds(pl.multiple_of(at * LANES, LANES), LANES)] = ref[pl.ds(i * 16, 16), :]


def shards(
    date_key,
    store_key,
    product_key,
    revenue,
    row_counts,
    date_years,
    date_flags,
    store_flags,
    product_flags,
    brand_words,
):
    gx, gy = lax.axis_index("gx"), lax.axis_index("gy")
    zl, x, y, c = gx // 16, gx // 4 % 4, gx % 4, gy % 2
    split = BRAND_ROWS * LANES
    low = jnp.concatenate([brand_words[:split], product_flags[:256]])
    pad = jnp.zeros(2 * split - LANES - brand_words.shape[0], jnp.int32)
    small_pad = jnp.zeros(LANES - 42, jnp.int32)
    high = jnp.concatenate(
        [
            brand_words[split:],
            pad,
            store_flags,
            date_years,
            date_flags,
            small_pad,
            product_flags[256:],
        ]
    )
    block = jnp.where(c == 0, low, high).reshape(BLOCK_ROWS, LANES)
    tables = gather_tables(block)
    where = jnp.stack([zl, x, y, c, row_counts[0]])
    facts = [a.reshape(-1, LANES) for a in (date_key, store_key, product_key, revenue)]
    partial = joined(where, *facts, tables)
    return sum_everywhere(partial, c)


def solution(mesh):
    placed = (P(AXES),) * 5 + (P("gx"),) * 5
    return jax.shard_map(shards, mesh=mesh, in_specs=placed, out_specs=P(), check_vma=False)
```

```python
import functools

import jax
import jax.numpy as jnp
from jax import lax
from jax.experimental import pallas as pl
from jax.experimental.pallas import tpu as pltpu
from jax.sharding import PartitionSpec as P

BRANDS = 1024
YEARS = 16
AXES = ("gx", "gy")
LANES = 128
BRAND_ROWS = 22
FLAG_ROWS = 2
BLOCK_ROWS = BRAND_ROWS + FLAG_ROWS
SPLIT_WORD = 2730
SMALL_LANE = 86
FAR_FIRST = (2, 3, 1)
FAR_FIRST_Z = (3, 2, 1)


def place_of(index):
    gx, gy = index // 4, index % 4
    return dict(z=gy // 2 * 4 + gx // 16, x=gx // 4 % 4, y=gx % 4, c=gy % 2)


def index_of(place):
    gx = place["z"] % 4 * 16 + place["x"] * 4 + place["y"]
    return gx * 4 + place["z"] // 4 * 2 + place["c"]


def swapped(value, axis, bits):
    pairs = []
    for source in range(256):
        place = place_of(source)
        place[axis] ^= bits
        pairs.append((source, index_of(place)))
    return lax.ppermute(value, AXES, pairs)


def from_four(value, axis):
    far = {bits: swapped(value, axis, bits) for bits in (FAR_FIRST_Z if axis == "z" else FAR_FIRST)}
    return [value] + [far[bits] for bits in (1, 2, 3)]


def lane_gather(rows, lanes):
    return jnp.take_along_axis(rows, lanes, axis=1, mode="promise_in_bounds")


def spread(ref, row):
    return jnp.broadcast_to(ref[pl.ds(row, 1), :], (8, LANES))


def packed_up(keep, meta, money):
    rows = keep.shape[0]
    above = lax.broadcasted_iota(jnp.int32, (rows, rows), 0) > lax.broadcasted_iota(
        jnp.int32, (rows, rows), 1
    )
    dropped = lax.dot_general(
        jnp.where(above, 1.0, 0.0).astype(jnp.bfloat16),
        (1 - keep).astype(jnp.float32).astype(jnp.bfloat16),
        (((1,), (0,)), ((), ())),
        preferred_element_type=jnp.float32,
    ).astype(jnp.int32)
    meta = jnp.where(keep == 1, meta | (dropped << 24), 0)
    for b in range(8):
        bit = jnp.int32((1 << (24 + b)) if b < 7 else -(2**31))
        coming = pltpu.roll(meta, rows - (1 << b), 0)
        coming_money = pltpu.roll(money, rows - (1 << b), 0)
        take = (coming & bit) != 0
        meta = jnp.where(take, coming, jnp.where((meta & bit) != 0, 0, meta))
        money = jnp.where(take, coming_money, money)
    return meta, money, jnp.sum(keep, axis=0, keepdims=True)


def join_kernel(where_ref, *refs):
    own, other, tables = refs[:4], refs[4:8], refs[8:12]
    out_ref, small_ref, keep_ref, meta_ref, money_scratch = refs[12:]
    zl, x, y, c = (where_ref[i] for i in range(4))
    lane = lax.broadcasted_iota(jnp.int32, (8, LANES), 1)
    sub = lax.broadcasted_iota(jnp.int32, (8, LANES), 0)
    rows = own[0].shape[0]

    lane_from = SMALL_LANE + jnp.where(
        sub == 0, lane & 31, jnp.where(sub == 1, 32 + (lane & 7), 40 + (lane & 1))
    )
    days = jnp.zeros((8, LANES), jnp.int32)
    for kz in range(4):
        oz = zl ^ kz
        years = jnp.zeros((8, LANES), jnp.int32)
        for kx in range(4):
            ox = x ^ kx
            stores = jnp.zeros((8, LANES), jnp.int32)
            for ky in range(4):
                oy = y ^ ky
                at = (ky * 4 + kz) * BLOCK_ROWS + BRAND_ROWS - 1
                moved = lane_gather(spread(tables[kx], at), lane_from)
                stores += jnp.where((lane >> 5) == oy, moved, 0)
                years += jnp.where((lane >> 3) == ox * 4 + oy, moved, 0)
                days += jnp.where((lane >> 1) == oz * 16 + ox * 4 + oy, moved, 0)
            small_ref[pl.ds(oz * 4 + ox, 1), :] = stores[0:1]
        small_ref[pl.ds(16 + oz, 1), :] = years[1:2]
    small_ref[pl.ds(20, 1), :] = days[2:3]

    def filter_block(refs, to, first):
        at = pl.ds(pl.multiple_of(first, 8), 8)
        date, store, product = (ref[at, :] for ref in refs[:3])
        year_lane, year_row = (date >> 3) & 127, date >> 10
        year_word = jnp.zeros_like(date)
        for i in range(4):
            year_word = jnp.where(
                year_row == i, lane_gather(spread(small_ref, 16 + i), year_lane), year_word
            )
        year = (year_word >> ((date & 7) * 4)) & 15
        passed = lane_gather(spread(small_ref, 20), date >> 5) >> (date & 31)
        store_lane, store_row = (store >> 5) & 127, store >> 12
        store_word = jnp.zeros_like(store)
        for i in range(16):
            store_word = jnp.where(
                store_row == i, lane_gather(spread(small_ref, i), store_lane), store_word
            )
        passed &= store_word >> (store & 31)
        here = (product >= 0) & (((product >> 13) & 1) == c)
        at = pl.ds(pl.multiple_of(to + first, 8), 8)
        keep_ref[at, :] = jnp.where(here, passed & 1, 0)
        meta_ref[at, :] = (product & 0xFFFFF) | (year << 20)

    def filter_blocks(turn, _):
        for u in range(2):
            for side, refs in enumerate((own, other)):
                filter_block(refs, side * rows, turn * 16 + u * 8)
        return 0

    lax.fori_loop(0, rows // 16, filter_blocks, 0)

    money_scratch[:rows, :] = own[3][...]
    money_scratch[rows:, :] = other[3][...]
    meta, money, left = packed_up(keep_ref[...], meta_ref[...], money_scratch[...])
    meta_ref[...] = meta
    money_scratch[...] = money
    keep_ref[...] = jnp.zeros_like(keep_ref)

    def search(rows_of, code, lanes, first, number, unroll):
        def step(turn, found):
            found = [list(f) for f in found]
            start = turn * (unroll * BLOCK_ROWS)
            code_now = [v - turn * (unroll * 128) for v in code]
            for u in range(unroll):
                for t in range(4):
                    for i in range(number):
                        row = spread(tables[t], start + (u * BLOCK_ROWS + first + i))
                        for q in range(rows_of):
                            at = i % 2
                            got = lane_gather(row, lanes[q])
                            found[q][at] = jnp.where(
                                code_now[q] == u * 128 + t * 32 + i, got, found[q][at]
                            )
            return tuple(tuple(f) for f in found)

        zero = jnp.zeros((8, LANES), jnp.int32)
        found = lax.fori_loop(0, 16 // unroll, step, ((zero, zero),) * rows_of)
        return [f[0] | f[1] for f in found]

    def code_of(product, row):
        oz, ox, oy = product >> 18, (product >> 16) & 3, (product >> 14) & 3
        return ((y ^ oy) * 4 + (zl ^ oz)) * 128 + (x ^ ox) * 32 + row

    def product_blocks(turn, _):
        ats = [pl.ds(pl.multiple_of(turn * 16 + u * 8, 8), 8) for u in range(2)]
        products = [meta_ref[at, :] & 0xFFFFF for at in ats]
        words = search(
            2,
            [code_of(p, (p >> 12) & 1) for p in products],
            [(p >> 5) & 127 for p in products],
            BRAND_ROWS,
            FLAG_ROWS,
            8,
        )
        for u, (at, product, word) in enumerate(zip(ats, products, words)):
            there = turn * 16 + u * 8 + sub < left
            keep_ref[at, :] = jnp.where(there, (word >> (product & 31)) & 1, 0)
        return 0

    lax.fori_loop(0, (jnp.max(left) + 15) // 16, product_blocks, 0)
    meta, money, left = packed_up(keep_ref[...], meta_ref[...] & 0xFFFFFF, money_scratch[...])
    meta_ref[...] = meta
    money_scratch[...] = money

    high_row = lax.broadcasted_iota(jnp.int32, (LANES, LANES), 0)
    out_ref[...] = jnp.zeros_like(out_ref)

    def add_block(block, _):
        at = pl.ds(pl.multiple_of(block * 8, 8), 8)
        meta = meta_ref[at, :]
        product, year = meta & 0xFFFFF, (meta >> 20) & 15
        local = product & 16383
        word = (local * 21846) >> 16
        digit = local - word * 3
        word -= c * SPLIT_WORD
        code = code_of(product, word >> 7)
        (found,) = search(1, [code], [word & 127], 0, BRAND_ROWS, 8)
        brand = (found >> (digit * 10)) & 1023
        amount = jnp.where(block * 8 + sub < left, money_scratch[at, :], 0.0)
        high = (brand >> 7) * YEARS + year
        low = brand & 127
        weighted, low_hot = [], []
        for s in range(8):
            weighted.append(
                jnp.where(high_row == high[s : s + 1, :], amount[s : s + 1, :], 0.0).astype(
                    jnp.bfloat16
                )
            )
            low_hot.append((high_row == low[s : s + 1, :]).astype(jnp.float32).astype(jnp.bfloat16))
        out_ref[...] += lax.dot_general(
            jnp.concatenate(weighted, axis=1),
            jnp.concatenate(low_hot, axis=1),
            (((1,), (1,)), ((), ())),
            preferred_element_type=jnp.float32,
        )
        return 0

    lax.fori_loop(0, (jnp.max(left) + 7) // 8, add_block, 0)


def joined(where, own, other, tables):
    vmem = pl.BlockSpec(memory_space=pltpu.VMEM)
    rows = 2 * own[0].shape[0]
    return pl.pallas_call(
        join_kernel,
        out_shape=jax.ShapeDtypeStruct((LANES, LANES), jnp.float32),
        in_specs=[pl.BlockSpec(memory_space=pltpu.SMEM)] + [vmem] * 12,
        out_specs=vmem,
        scratch_shapes=[
            pltpu.VMEM((24, LANES), jnp.int32),
            pltpu.VMEM((rows, LANES), jnp.int32),
            pltpu.VMEM((rows, LANES), jnp.int32),
            pltpu.VMEM((rows, LANES), jnp.float32),
        ],
        cost_estimate=pl.CostEstimate(flops=10**8, bytes_accessed=10**6, transcendentals=0),
        compiler_params=pltpu.CompilerParams(vmem_limit_bytes=8 * 2**20),
    )(where, *own, *other, *tables)


def gather_tables(block):
    line = jnp.concatenate(from_four(block, "z"), axis=0)
    return from_four(jnp.concatenate(from_four(line, "y"), axis=0), "x")


def four_added(value, axis):
    a, b, c, d = from_four(value, axis)
    return (a + b) + (c + d)


def sum_everywhere(partial, c):
    def half(at):
        return lax.dynamic_slice_in_dim(partial, at * 64, 64, 0)

    total = half(c) + swapped(half(1 - c), "c", 1)
    for axis in ("x", "y", "z"):
        total = four_added(total, axis)
    total = total + swapped(total, "z", 7)
    return pl.pallas_call(
        lay_kernel,
        out_shape=jax.ShapeDtypeStruct((YEARS, BRANDS), jnp.float32),
        in_specs=[pl.BlockSpec(memory_space=pltpu.SMEM)]
        + [pl.BlockSpec(memory_space=pltpu.VMEM)] * 2,
        out_specs=pl.BlockSpec(memory_space=pltpu.VMEM),
        compiler_params=pltpu.CompilerParams(vmem_limit_bytes=2**20),
    )(c[None], total, swapped(total, "c", 1))


def lay_kernel(c_ref, mine_ref, other_ref, out_ref):
    for side, ref in enumerate((mine_ref, other_ref)):
        for i in range(4):
            at = (c_ref[0] ^ side) * 4 + i
            out_ref[:, pl.ds(pl.multiple_of(at * LANES, LANES), LANES)] = ref[pl.ds(i * 16, 16), :]


def shards(
    date_key,
    store_key,
    product_key,
    revenue,
    row_counts,
    date_years,
    date_flags,
    store_flags,
    product_flags,
    brand_words,
):
    gx, gy = lax.axis_index("gx"), lax.axis_index("gy")
    zl, x, y, c = gx >> 4, (gx >> 2) & 3, gx & 3, gy & 1
    brand_some = brand_words.shape[0] - SPLIT_WORD
    block = jnp.concatenate(
        [
            lax.dynamic_slice_in_dim(brand_words, c * SPLIT_WORD, brand_some, 0),
            jnp.zeros(BRAND_ROWS * LANES - (LANES - SMALL_LANE) - brand_some, jnp.int32),
            store_flags,
            date_years,
            date_flags,
            lax.dynamic_slice_in_dim(product_flags, c * 256, 256, 0),
        ]
    ).reshape(BLOCK_ROWS, LANES)
    live = lax.iota(jnp.int32, product_key.shape[0]) < row_counts[0]
    own = [
        a.reshape(-1, LANES)
        for a in (
            date_key,
            store_key,
            jnp.where(live, product_key, -1),
            revenue.astype(jnp.float32),
        )
    ]
    other = [swapped(a, "c", 1) for a in own]
    tables = gather_tables(block)
    partial = joined(jnp.stack([zl, x, y, c]), own, other, tables)
    return sum_everywhere(partial, c)


def solution(mesh):
    placed = (P(AXES),) * 5 + (P("gx"),) * 5
    return jax.shard_map(shards, mesh=mesh, in_specs=placed, out_specs=P(), check_vma=False)
```

```python
import functools

import jax
import jax.numpy as jnp
from jax import lax
from jax.experimental import pallas as pl
from jax.experimental.pallas import tpu as pltpu
from jax.sharding import PartitionSpec as P

BRANDS = 1024
YEARS = 16
AXES = ("gx", "gy")
LANES = 128
BRAND_ROWS = 22
FLAG_ROWS = 2
BLOCK_ROWS = BRAND_ROWS + FLAG_ROWS
SPLIT_ROW = 21
SMALL_LANE = 86


def place_of(index):
    gx, gy = index // 4, index % 4
    return dict(z=gy // 2 * 4 + gx // 16, x=gx // 4 % 4, y=gx % 4, c=gy % 2)


def index_of(place):
    gx = place["z"] % 4 * 16 + place["x"] * 4 + place["y"]
    return gx * 4 + place["z"] // 4 * 2 + place["c"]


def moved(value, move):
    pairs = []
    for source in range(256):
        place = place_of(source)
        move(place)
        pairs.append((source, index_of(place)))
    return lax.ppermute(value, AXES, pairs)


def swapped(value, axis, bits):
    def move(place):
        place[axis] ^= bits

    return moved(value, move)


def shifted(value, axis, steps):
    def move(place):
        place[axis] = (place[axis] + steps) % 4

    return moved(value, move)


def from_four(value, axis):
    if axis == "z":
        far = {bits: swapped(value, axis, bits) for bits in (2, 3, 1)}
    else:
        far = {steps: shifted(value, axis, steps) for steps in (1, 3, 2)}
    return [value] + [far[k] for k in (1, 2, 3)]


def lane_gather(rows, lanes):
    return jnp.take_along_axis(rows, lanes, axis=1, mode="promise_in_bounds")


def spread(ref, row):
    return jnp.broadcast_to(ref[pl.ds(row, 1), :], (8, LANES))


def packed_up(keep, meta, money):
    rows = keep.shape[0]
    above = lax.broadcasted_iota(jnp.int32, (rows, rows), 0) > lax.broadcasted_iota(
        jnp.int32, (rows, rows), 1
    )
    dropped = lax.dot_general(
        jnp.where(above, 1.0, 0.0).astype(jnp.bfloat16),
        (1 - keep).astype(jnp.float32).astype(jnp.bfloat16),
        (((1,), (0,)), ((), ())),
        preferred_element_type=jnp.float32,
    ).astype(jnp.int32)
    meta = jnp.where(keep == 1, meta | (dropped << 24), 0)
    for b in range(8):
        bit = jnp.int32((1 << (24 + b)) if b < 7 else -(2**31))
        coming = pltpu.roll(meta, rows - (1 << b), 0)
        coming_money = pltpu.roll(money, rows - (1 << b), 0)
        take = (coming & bit) != 0
        meta = jnp.where(take, coming, jnp.where((meta & bit) != 0, 0, meta))
        money = jnp.where(take, coming_money, money)
    return meta, money, jnp.sum(keep, axis=0, keepdims=True)


def join_kernel(where_ref, *refs):
    own, other, tables = refs[:4], refs[4:8], refs[8:12]
    out_ref, small_ref, keep_ref, meta_ref, money_scratch = refs[12:]
    zl, x, y, c = (where_ref[i] for i in range(4))
    lane = lax.broadcasted_iota(jnp.int32, (8, LANES), 1)
    sub = lax.broadcasted_iota(jnp.int32, (8, LANES), 0)
    rows = own[0].shape[0]

    lane_from = SMALL_LANE + jnp.where(
        sub == 0, lane & 31, jnp.where(sub == 1, 32 + (lane & 7), 40 + (lane & 1))
    )
    days = jnp.zeros((8, LANES), jnp.int32)
    for kz in range(4):
        oz = zl ^ kz
        years = jnp.zeros((8, LANES), jnp.int32)
        for kx in range(4):
            ox = (x - kx) & 3
            stores = jnp.zeros((8, LANES), jnp.int32)
            for ky in range(4):
                oy = (y - ky) & 3
                at = (ky * 4 + kz) * BLOCK_ROWS + BRAND_ROWS - 1
                moved = lane_gather(spread(tables[kx], at), lane_from)
                stores += jnp.where((lane >> 5) == oy, moved, 0)
                years += jnp.where((lane >> 3) == ox * 4 + oy, moved, 0)
                days += jnp.where((lane >> 1) == oz * 16 + ox * 4 + oy, moved, 0)
            small_ref[pl.ds(oz * 4 + ox, 1), :] = stores[0:1]
        small_ref[pl.ds(16 + oz, 1), :] = years[1:2]
    small_ref[pl.ds(20, 1), :] = days[2:3]

    def filter_block(refs, to, first):
        at = pl.ds(pl.multiple_of(first, 8), 8)
        date, store, product = (ref[at, :] for ref in refs[:3])
        year_lane, year_row = (date >> 3) & 127, date >> 10
        year_word = jnp.zeros_like(date)
        for i in range(4):
            year_word = jnp.where(
                year_row == i, lane_gather(spread(small_ref, 16 + i), year_lane), year_word
            )
        year = (year_word >> ((date & 7) * 4)) & 15
        passed = lane_gather(spread(small_ref, 20), date >> 5) >> (date & 31)
        store_lane, store_row = (store >> 5) & 127, store >> 12
        store_word = jnp.zeros_like(store)
        for i in range(16):
            store_word = jnp.where(
                store_row == i, lane_gather(spread(small_ref, i), store_lane), store_word
            )
        passed &= store_word >> (store & 31)
        here = (product >= 0) & (((product >> 13) & 1) == c)
        at = pl.ds(pl.multiple_of(to + first, 8), 8)
        keep_ref[at, :] = jnp.where(here, passed & 1, 0)
        meta_ref[at, :] = (product & 0xFFFFF) | (year << 20)

    def filter_blocks(turn, _):
        for u in range(2):
            for side, refs in enumerate((own, other)):
                filter_block(refs, side * rows, turn * 16 + u * 8)
        return 0

    lax.fori_loop(0, rows // 16, filter_blocks, 0)

    money_scratch[:rows, :] = own[3][...]
    money_scratch[rows:, :] = other[3][...]
    meta, money, left = packed_up(keep_ref[...], meta_ref[...], money_scratch[...])
    meta_ref[...] = meta
    money_scratch[...] = money
    keep_ref[...] = jnp.zeros_like(keep_ref)

    def search(rows_of, code, lanes, first, number, unroll):
        def step(turn, found):
            found = [list(f) for f in found]
            start = turn * (unroll * BLOCK_ROWS)
            code_now = [v - turn * (unroll * 128) for v in code]
            for u in range(unroll):
                for t in range(4):
                    for i in range(number):
                        row = spread(tables[t], start + (u * BLOCK_ROWS + first + i))
                        for q in range(rows_of):
                            at = i % 2
                            got = lane_gather(row, lanes[q])
                            found[q][at] = jnp.where(
                                code_now[q] == u * 128 + t * 32 + i, got, found[q][at]
                            )
            return tuple(tuple(f) for f in found)

        zero = jnp.zeros((8, LANES), jnp.int32)
        found = lax.fori_loop(0, 16 // unroll, step, ((zero, zero),) * rows_of)
        return [f[0] | f[1] for f in found]

    def code_of(product, row):
        oz, ox, oy = product >> 18, (product >> 16) & 3, (product >> 14) & 3
        return (((y - oy) & 3) * 4 + (zl ^ oz)) * 128 + ((x - ox) & 3) * 32 + row

    def product_blocks(turn, _):
        ats = [pl.ds(pl.multiple_of(turn * 16 + u * 8, 8), 8) for u in range(2)]
        products = [meta_ref[at, :] & 0xFFFFF for at in ats]
        words = search(
            2,
            [code_of(p, (p >> 12) & 1) for p in products],
            [(p >> 5) & 127 for p in products],
            BRAND_ROWS,
            FLAG_ROWS,
            8,
        )
        for u, (at, product, word) in enumerate(zip(ats, products, words)):
            there = turn * 16 + u * 8 + sub < left
            keep_ref[at, :] = jnp.where(there, (word >> (product & 31)) & 1, 0)
        return 0

    lax.fori_loop(0, (jnp.max(left) + 15) // 16, product_blocks, 0)
    meta, money, left = packed_up(keep_ref[...], meta_ref[...] & 0xFFFFFF, money_scratch[...])
    meta_ref[...] = meta
    money_scratch[...] = money

    high_row = lax.broadcasted_iota(jnp.int32, (LANES, LANES), 0)
    out_ref[...] = jnp.zeros_like(out_ref)

    def add_block(block, _):
        at = pl.ds(pl.multiple_of(block * 8, 8), 8)
        meta = meta_ref[at, :]
        product, year = meta & 0xFFFFF, (meta >> 20) & 15
        local = product & 16383
        word = (local * 21846) >> 16
        digit = local - word * 3
        code = code_of(product, (word >> 7) - c * SPLIT_ROW)
        (found,) = search(1, [code], [word & 127], 0, BRAND_ROWS, 8)
        brand = (found >> (digit * 10)) & 1023
        amount = jnp.where(block * 8 + sub < left, money_scratch[at, :], 0.0)
        high = (brand >> 7) * YEARS + year
        low = brand & 127
        weighted, low_hot = [], []
        for s in range(8):
            weighted.append(
                jnp.where(high_row == high[s : s + 1, :], amount[s : s + 1, :], 0.0).astype(
                    jnp.bfloat16
                )
            )
            low_hot.append((high_row == low[s : s + 1, :]).astype(jnp.float32).astype(jnp.bfloat16))
        out_ref[...] += lax.dot_general(
            jnp.concatenate(weighted, axis=1),
            jnp.concatenate(low_hot, axis=1),
            (((1,), (1,)), ((), ())),
            preferred_element_type=jnp.float32,
        )
        return 0

    lax.fori_loop(0, (jnp.max(left) + 7) // 8, add_block, 0)


def joined(where, own, other, tables):
    vmem = pl.BlockSpec(memory_space=pltpu.VMEM)
    rows = 2 * own[0].shape[0]
    return pl.pallas_call(
        join_kernel,
        out_shape=jax.ShapeDtypeStruct((LANES, LANES), jnp.float32),
        in_specs=[pl.BlockSpec(memory_space=pltpu.SMEM)] + [vmem] * 12,
        out_specs=vmem,
        scratch_shapes=[
            pltpu.VMEM((24, LANES), jnp.int32),
            pltpu.VMEM((rows, LANES), jnp.int32),
            pltpu.VMEM((rows, LANES), jnp.int32),
            pltpu.VMEM((rows, LANES), jnp.float32),
        ],
        cost_estimate=pl.CostEstimate(flops=10**8, bytes_accessed=10**6, transcendentals=0),
        compiler_params=pltpu.CompilerParams(vmem_limit_bytes=8 * 2**20),
    )(where, *own, *other, *tables)


def half_kernel(c_ref, packed_ref, out_ref):
    for half in range(2):

        @pl.when(c_ref[0] == half)
        def _(half=half):
            out_ref[:BRAND_ROWS, :] = packed_ref[pl.ds(half * SPLIT_ROW, BRAND_ROWS), :]
            out_ref[BRAND_ROWS:, :] = packed_ref[pl.ds(43 + half * FLAG_ROWS, FLAG_ROWS), :]

    lane = lax.broadcasted_iota(jnp.int32, (1, LANES), 1)
    last = pl.ds(BRAND_ROWS - 1, 1)
    out_ref[last, :] = jnp.where(lane < SMALL_LANE, out_ref[last, :], packed_ref[pl.ds(42, 1), :])


def half_of(c, packed):
    vmem = pl.BlockSpec(memory_space=pltpu.VMEM)
    return pl.pallas_call(
        half_kernel,
        out_shape=jax.ShapeDtypeStruct((BLOCK_ROWS, LANES), jnp.int32),
        in_specs=[pl.BlockSpec(memory_space=pltpu.SMEM), vmem],
        out_specs=vmem,
        compiler_params=pltpu.CompilerParams(vmem_limit_bytes=2**20),
    )(c[None], packed)


def gather_tables(block):
    line = jnp.concatenate(from_four(block, "z"), axis=0)
    return from_four(jnp.concatenate(from_four(line, "y"), axis=0), "x")


def four_added(value, axis):
    a, b, c, d = from_four(value, axis)
    return (a + b) + (c + d) if axis == "z" else (a + c) + (b + d)


def sum_everywhere(partial, c):
    def half(at):
        return lax.dynamic_slice_in_dim(partial, at * 64, 64, 0)

    total = half(c) + swapped(half(1 - c), "c", 1)
    for axis in ("x", "y", "z"):
        total = four_added(total, axis)
    total = total + swapped(total, "z", 7)
    return pl.pallas_call(
        lay_kernel,
        out_shape=jax.ShapeDtypeStruct((YEARS, BRANDS), jnp.float32),
        in_specs=[pl.BlockSpec(memory_space=pltpu.SMEM)]
        + [pl.BlockSpec(memory_space=pltpu.VMEM)] * 2,
        out_specs=pl.BlockSpec(memory_space=pltpu.VMEM),
        compiler_params=pltpu.CompilerParams(vmem_limit_bytes=2**20),
    )(c[None], total, swapped(total, "c", 1))


def lay_kernel(c_ref, mine_ref, other_ref, out_ref):
    for side, ref in enumerate((mine_ref, other_ref)):
        for i in range(4):
            at = (c_ref[0] ^ side) * 4 + i
            out_ref[:, pl.ds(pl.multiple_of(at * LANES, LANES), LANES)] = ref[pl.ds(i * 16, 16), :]


def shards(
    date_key,
    store_key,
    product_key,
    revenue,
    row_counts,
    date_years,
    date_flags,
    store_flags,
    product_flags,
    brand_words,
):
    gx, gy = lax.axis_index("gx"), lax.axis_index("gy")
    zl, x, y, c = gx >> 4, (gx >> 2) & 3, gx & 3, gy & 1
    packed = jnp.concatenate(
        [brand_words[: 43 * LANES - 42], store_flags, date_years, date_flags, product_flags]
    ).reshape(47, LANES)
    block = half_of(c, packed)
    live = lax.iota(jnp.int32, product_key.shape[0]) < row_counts[0]
    own = [
        a.reshape(-1, LANES)
        for a in (
            date_key,
            store_key,
            jnp.where(live, product_key, -1),
            revenue.astype(jnp.float32),
        )
    ]
    other = [swapped(a, "c", 1) for a in own]
    tables = gather_tables(block)
    partial = joined(jnp.stack([zl, x, y, c]), own, other, tables)
    return sum_everywhere(partial, c)


def solution(mesh):
    placed = (P(AXES),) * 5 + (P("gx"),) * 5
    return jax.shard_map(shards, mesh=mesh, in_specs=placed, out_specs=P(), check_vma=False)
```

```python
import functools

import jax
import jax.numpy as jnp
from jax import lax
from jax.experimental import pallas as pl
from jax.experimental.pallas import tpu as pltpu
from jax.sharding import PartitionSpec as P

BRANDS = 1024
YEARS = 16
AXES = ("gx", "gy")
LANES = 128
BRAND_ROWS = 22
FLAG_ROWS = 2
BLOCK_ROWS = BRAND_ROWS + FLAG_ROWS
SPLIT_ROW = 21
SMALL_LANE = 86


def place_of(index):
    gx, gy = index // 4, index % 4
    return dict(z=gy // 2 * 4 + gx // 16, x=gx // 4 % 4, y=gx % 4, c=gy % 2)


def index_of(place):
    gx = place["z"] % 4 * 16 + place["x"] * 4 + place["y"]
    return gx * 4 + place["z"] // 4 * 2 + place["c"]


def moved(value, move):
    pairs = []
    for source in range(256):
        place = place_of(source)
        move(place)
        pairs.append((source, index_of(place)))
    return lax.ppermute(value, AXES, pairs)


def swapped(value, axis, bits):
    def move(place):
        place[axis] ^= bits

    return moved(value, move)


def shifted(value, axis, steps):
    def move(place):
        place[axis] = place[axis] // 4 * 4 + (place[axis] + steps) % 4

    return moved(value, move)


def from_behind(value, axis, order):
    far = {steps: shifted(value, axis, steps) for steps in order}
    return [value] + [far[k] for k in (1, 2, 3)]


def lane_gather(rows, lanes):
    return jnp.take_along_axis(rows, lanes, axis=1, mode="promise_in_bounds")


def spread(ref, row):
    return jnp.broadcast_to(ref[pl.ds(row, 1), :], (8, LANES))


def packed_up(keep, meta, money):
    rows = keep.shape[0]
    above = lax.broadcasted_iota(jnp.int32, (rows, rows), 0) > lax.broadcasted_iota(
        jnp.int32, (rows, rows), 1
    )
    dropped = lax.dot_general(
        jnp.where(above, 1.0, 0.0).astype(jnp.bfloat16),
        (1 - keep).astype(jnp.float32).astype(jnp.bfloat16),
        (((1,), (0,)), ((), ())),
        preferred_element_type=jnp.float32,
    ).astype(jnp.int32)
    meta = jnp.where(keep == 1, meta | (dropped << 24), 0)
    for b in range((rows - 1).bit_length()):
        bit = jnp.int32((1 << (24 + b)) if b < 7 else -(2**31))
        coming = pltpu.roll(meta, rows - (1 << b), 0)
        coming_money = pltpu.roll(money, rows - (1 << b), 0)
        take = (coming & bit) != 0
        meta = jnp.where(take, coming, jnp.where((meta & bit) != 0, 0, meta))
        money = jnp.where(take, coming_money, money)
    return meta, money, jnp.sum(keep, axis=0, keepdims=True)


def join_kernel(where_ref, *refs):
    own, other, tables = refs[:4], refs[4:8], refs[8:12]
    out_ref, small_ref, keep_ref, meta_ref, money_scratch = refs[12:]
    zl, x, y, c = (where_ref[i] for i in range(4))
    lane = lax.broadcasted_iota(jnp.int32, (8, LANES), 1)
    sub = lax.broadcasted_iota(jnp.int32, (8, LANES), 0)
    rows = own[0].shape[0]

    lane_from = SMALL_LANE + jnp.where(
        sub == 0, lane & 31, jnp.where(sub == 1, 32 + (lane & 7), 40 + (lane & 1))
    )
    days = jnp.zeros((8, LANES), jnp.int32)
    for kz in range(4):
        oz = (zl - kz) & 3
        years = jnp.zeros((8, LANES), jnp.int32)
        for kx in range(4):
            ox = (x - kx) & 3
            stores = jnp.zeros((8, LANES), jnp.int32)
            for ky in range(4):
                oy = (y - ky) & 3
                at = (ky * 4 + kz) * BLOCK_ROWS + BRAND_ROWS - 1
                moved = lane_gather(spread(tables[kx], at), lane_from)
                stores += jnp.where((lane >> 5) == oy, moved, 0)
                years += jnp.where((lane >> 3) == ox * 4 + oy, moved, 0)
                days += jnp.where((lane >> 1) == oz * 16 + ox * 4 + oy, moved, 0)
            small_ref[pl.ds(oz * 4 + ox, 1), :] = stores[0:1]
        small_ref[pl.ds(16 + oz, 1), :] = years[1:2]
    small_ref[pl.ds(20, 1), :] = days[2:3]

    def filter_block(refs, to, first):
        at = pl.ds(pl.multiple_of(first, 8), 8)
        date, store, product = (ref[at, :] for ref in refs[:3])
        year_lane, year_row = (date >> 3) & 127, date >> 10
        year_word = jnp.zeros_like(date)
        for i in range(4):
            year_word = jnp.where(
                year_row == i, lane_gather(spread(small_ref, 16 + i), year_lane), year_word
            )
        year = (year_word >> ((date & 7) * 4)) & 15
        passed = lane_gather(spread(small_ref, 20), date >> 5) >> (date & 31)
        store_lane, store_row = (store >> 5) & 127, store >> 12
        store_word = jnp.zeros_like(store)
        for i in range(16):
            store_word = jnp.where(
                store_row == i, lane_gather(spread(small_ref, i), store_lane), store_word
            )
        passed &= store_word >> (store & 31)
        here = (product >= 0) & (((product >> 13) & 1) == c)
        at = pl.ds(pl.multiple_of(to + first, 8), 8)
        keep_ref[at, :] = jnp.where(here, passed & 1, 0)
        meta_ref[at, :] = (product & 0xFFFFF) | (year << 20)

    def filter_blocks(turn, _):
        for u in range(4):
            for side, refs in enumerate((own, other)):
                filter_block(refs, side * rows, turn * 32 + u * 8)
        return 0

    lax.fori_loop(0, rows // 32, filter_blocks, 0)

    money_scratch[:rows, :] = own[3][...]
    money_scratch[rows:, :] = other[3][...]
    meta, money, left = packed_up(keep_ref[...], meta_ref[...], money_scratch[...])
    meta_ref[...] = meta
    money_scratch[...] = money
    keep_ref[...] = jnp.zeros_like(keep_ref)

    def search(rows_of, code, lanes, first, number, unroll):
        def step(turn, found):
            found = [list(f) for f in found]
            start = turn * (unroll * BLOCK_ROWS)
            code_now = [v - turn * (unroll * 128) for v in code]
            for u in range(unroll):
                for t in range(4):
                    for i in range(number):
                        row = spread(tables[t], start + (u * BLOCK_ROWS + first + i))
                        for q in range(rows_of):
                            at = i % 2
                            got = lane_gather(row, lanes[q])
                            found[q][at] = jnp.where(
                                code_now[q] == u * 128 + t * 32 + i, got, found[q][at]
                            )
            return tuple(tuple(f) for f in found)

        zero = jnp.zeros((8, LANES), jnp.int32)
        found = lax.fori_loop(0, 16 // unroll, step, ((zero, zero),) * rows_of)
        return [f[0] | f[1] for f in found]

    def code_of(product, row):
        oz, ox, oy = product >> 18, (product >> 16) & 3, (product >> 14) & 3
        return (((y - oy) & 3) * 4 + ((zl - oz) & 3)) * 128 + ((x - ox) & 3) * 32 + row

    def product_blocks(turn, _):
        ats = [pl.ds(pl.multiple_of(turn * 16 + u * 8, 8), 8) for u in range(2)]
        products = [meta_ref[at, :] & 0xFFFFF for at in ats]
        words = search(
            2,
            [code_of(p, (p >> 12) & 1) for p in products],
            [(p >> 5) & 127 for p in products],
            BRAND_ROWS,
            FLAG_ROWS,
            8,
        )
        for u, (at, product, word) in enumerate(zip(ats, products, words)):
            there = turn * 16 + u * 8 + sub < left
            keep_ref[at, :] = jnp.where(there, (word >> (product & 31)) & 1, 0)
        return 0

    most = jnp.max(left)
    lax.fori_loop(0, (most + 15) // 16, product_blocks, 0)

    def pack_first(rows):
        meta, money, left = packed_up(
            keep_ref[:rows, :], meta_ref[:rows, :] & 0xFFFFFF, money_scratch[:rows, :]
        )
        meta_ref[:rows, :] = meta
        money_scratch[:rows, :] = money
        return left

    left = lax.cond(most <= 64, lambda: pack_first(64), lambda: pack_first(2 * rows))

    high_row = lax.broadcasted_iota(jnp.int32, (LANES, LANES), 0)
    out_ref[...] = jnp.zeros_like(out_ref)

    def add_block(block, _):
        at = pl.ds(pl.multiple_of(block * 8, 8), 8)
        meta = meta_ref[at, :]
        product, year = meta & 0xFFFFF, (meta >> 20) & 15
        local = product & 16383
        word = (local * 21846) >> 16
        digit = local - word * 3
        code = code_of(product, (word >> 7) - c * SPLIT_ROW)
        (found,) = search(1, [code], [word & 127], 0, BRAND_ROWS, 16)
        brand = (found >> (digit * 10)) & 1023
        amount = jnp.where(block * 8 + sub < left, money_scratch[at, :], 0.0)
        high = (brand >> 7) * YEARS + year
        low = brand & 127
        weighted, low_hot = [], []
        for s in range(8):
            weighted.append(
                jnp.where(high_row == high[s : s + 1, :], amount[s : s + 1, :], 0.0).astype(
                    jnp.bfloat16
                )
            )
            low_hot.append((high_row == low[s : s + 1, :]).astype(jnp.float32).astype(jnp.bfloat16))
        out_ref[...] += lax.dot_general(
            jnp.concatenate(weighted, axis=1),
            jnp.concatenate(low_hot, axis=1),
            (((1,), (1,)), ((), ())),
            preferred_element_type=jnp.float32,
        )
        return 0

    lax.fori_loop(0, (jnp.max(left) + 7) // 8, add_block, 0)


def joined(where, own, other, tables):
    vmem = pl.BlockSpec(memory_space=pltpu.VMEM)
    rows = 2 * own[0].shape[0]
    return pl.pallas_call(
        join_kernel,
        out_shape=jax.ShapeDtypeStruct((LANES, LANES), jnp.float32),
        in_specs=[pl.BlockSpec(memory_space=pltpu.SMEM)] + [vmem] * 12,
        out_specs=vmem,
        scratch_shapes=[
            pltpu.VMEM((24, LANES), jnp.int32),
            pltpu.VMEM((rows, LANES), jnp.int32),
            pltpu.VMEM((rows, LANES), jnp.int32),
            pltpu.VMEM((rows, LANES), jnp.float32),
        ],
        cost_estimate=pl.CostEstimate(flops=10**8, bytes_accessed=10**6, transcendentals=0),
        compiler_params=pltpu.CompilerParams(
            vmem_limit_bytes=8 * 2**20
        ),
    )(where, *own, *other, *tables)


def half_kernel(c_ref, packed_ref, out_ref):
    for half in range(2):

        @pl.when(c_ref[0] == half)
        def _(half=half):
            out_ref[:BRAND_ROWS, :] = packed_ref[pl.ds(half * SPLIT_ROW, BRAND_ROWS), :]
            out_ref[BRAND_ROWS:, :] = packed_ref[pl.ds(43 + half * FLAG_ROWS, FLAG_ROWS), :]

    lane = lax.broadcasted_iota(jnp.int32, (1, LANES), 1)
    last = pl.ds(BRAND_ROWS - 1, 1)
    out_ref[last, :] = jnp.where(lane < SMALL_LANE, out_ref[last, :], packed_ref[pl.ds(42, 1), :])


def half_of(c, packed):
    vmem = pl.BlockSpec(memory_space=pltpu.VMEM)
    return pl.pallas_call(
        half_kernel,
        out_shape=jax.ShapeDtypeStruct((BLOCK_ROWS, LANES), jnp.int32),
        in_specs=[pl.BlockSpec(memory_space=pltpu.SMEM), vmem],
        out_specs=vmem,
        compiler_params=pltpu.CompilerParams(vmem_limit_bytes=2**20),
    )(c[None], packed)


def gather_tables(block):
    line = jnp.concatenate(from_behind(block, "z", (1, 2, 3)), axis=0)
    plane = jnp.concatenate(from_behind(line, "y", (1, 3, 2)), axis=0)
    return from_behind(plane, "x", (1, 3, 2))


def four_added(value, axis):
    if axis == "z":
        c, b, a = (swapped(value, axis, bits) for bits in (3, 2, 1))
        return (value + a) + (b + c)
    a, b, c, d = from_behind(value, axis, (1, 3, 2))
    return (a + c) + (b + d)


def sum_everywhere(partial, c):
    def half(at):
        return lax.dynamic_slice_in_dim(partial, at * 64, 64, 0)

    total = half(c) + swapped(half(1 - c), "c", 1)
    for axis in ("x", "y", "z"):
        total = four_added(total, axis)
    total = total + swapped(total, "z", 7)
    return pl.pallas_call(
        lay_kernel,
        out_shape=jax.ShapeDtypeStruct((YEARS, BRANDS), jnp.float32),
        in_specs=[pl.BlockSpec(memory_space=pltpu.SMEM)]
        + [pl.BlockSpec(memory_space=pltpu.VMEM)] * 2,
        out_specs=pl.BlockSpec(memory_space=pltpu.VMEM),
        compiler_params=pltpu.CompilerParams(vmem_limit_bytes=2**20),
    )(c[None], total, swapped(total, "c", 1))


def lay_kernel(c_ref, mine_ref, other_ref, out_ref):
    for side, ref in enumerate((mine_ref, other_ref)):
        for i in range(4):
            at = (c_ref[0] ^ side) * 4 + i
            out_ref[:, pl.ds(pl.multiple_of(at * LANES, LANES), LANES)] = ref[pl.ds(i * 16, 16), :]


def shards(
    date_key,
    store_key,
    product_key,
    revenue,
    row_counts,
    date_years,
    date_flags,
    store_flags,
    product_flags,
    brand_words,
):
    gx, gy = lax.axis_index("gx"), lax.axis_index("gy")
    zl, x, y, c = gx >> 4, (gx >> 2) & 3, gx & 3, gy & 1
    packed = jnp.concatenate(
        [brand_words[: 43 * LANES - 42], store_flags, date_years, date_flags, product_flags]
    ).reshape(47, LANES)
    block = half_of(c, packed)
    live = lax.iota(jnp.int32, product_key.shape[0]) < row_counts[0]
    own = [
        a.reshape(-1, LANES)
        for a in (
            date_key,
            store_key,
            jnp.where(live, product_key, -1),
            revenue.astype(jnp.float32),
        )
    ]
    other = [swapped(a, "c", 1) for a in own]
    tables = gather_tables(block)
    partial = joined(jnp.stack([zl, x, y, c]), own, other, tables)
    return sum_everywhere(partial, c)


def solution(mesh):
    placed = (P(AXES),) * 5 + (P("gx"),) * 5
    return jax.shard_map(shards, mesh=mesh, in_specs=placed, out_specs=P(), check_vma=False)
```

```python
import functools

import jax
import jax.numpy as jnp
from jax import lax
from jax.experimental import pallas as pl
from jax.experimental.pallas import tpu as pltpu
from jax.sharding import PartitionSpec as P

BRANDS = 1024
YEARS = 16
AXES = ("gx", "gy")
LANES = 128
BRAND_ROWS = 22
FLAG_ROWS = 2
BLOCK_ROWS = BRAND_ROWS + FLAG_ROWS
SPLIT_ROW = 21
SMALL_LANE = 86


def place_of(index):
    gx, gy = index // 4, index % 4
    return dict(z=gy // 2 * 4 + gx // 16, x=gx // 4 % 4, y=gx % 4, c=gy % 2)


def index_of(place):
    gx = place["z"] % 4 * 16 + place["x"] * 4 + place["y"]
    return gx * 4 + place["z"] // 4 * 2 + place["c"]


def moved(value, move):
    pairs = []
    for source in range(256):
        place = place_of(source)
        move(place)
        pairs.append((source, index_of(place)))
    return lax.ppermute(value, AXES, pairs)


def swapped(value, axis, bits):
    def move(place):
        place[axis] ^= bits

    return moved(value, move)


def shifted(value, axis, steps):
    def move(place):
        place[axis] = place[axis] // 4 * 4 + (place[axis] + steps) % 4

    return moved(value, move)


def from_behind(value, axis, order):
    far = {steps: shifted(value, axis, steps) for steps in order}
    return [value] + [far[k] for k in (1, 2, 3)]


def lane_gather(rows, lanes):
    return jnp.take_along_axis(rows, lanes, axis=1, mode="promise_in_bounds")


def spread(ref, row):
    return jnp.broadcast_to(ref[pl.ds(row, 1), :], (8, LANES))


def packed_up(keep, meta, money):
    rows = keep.shape[0]
    above = lax.broadcasted_iota(jnp.int32, (rows, rows), 0) > lax.broadcasted_iota(
        jnp.int32, (rows, rows), 1
    )
    dropped = lax.dot_general(
        jnp.where(above, 1.0, 0.0).astype(jnp.bfloat16),
        (1 - keep).astype(jnp.float32).astype(jnp.bfloat16),
        (((1,), (0,)), ((), ())),
        preferred_element_type=jnp.float32,
    ).astype(jnp.int32)
    meta = jnp.where(keep == 1, meta | (dropped << 24), 0)
    for b in range((rows - 1).bit_length()):
        bit = jnp.int32((1 << (24 + b)) if b < 7 else -(2**31))
        coming = pltpu.roll(meta, rows - (1 << b), 0)
        coming_money = pltpu.roll(money, rows - (1 << b), 0)
        take = (coming & bit) != 0
        meta = jnp.where(take, coming, jnp.where((meta & bit) != 0, 0, meta))
        money = jnp.where(take, coming_money, money)
    return meta, money, jnp.sum(keep, axis=0, keepdims=True)


def join_kernel(where_ref, *refs):
    own, other, tables = refs[:4], refs[4:8], refs[8:12]
    out_ref, small_ref, keep_ref, meta_ref, money_scratch, metas_ref, moneys_ref = refs[12:]
    zl, x, y, c = (where_ref[i] for i in range(4))
    lane = lax.broadcasted_iota(jnp.int32, (8, LANES), 1)
    sub = lax.broadcasted_iota(jnp.int32, (8, LANES), 0)
    rows = own[0].shape[0]

    lane_from = SMALL_LANE + jnp.where(
        sub == 0, lane & 31, jnp.where(sub == 1, 32 + (lane & 7), 40 + (lane & 1))
    )
    days = jnp.zeros((8, LANES), jnp.int32)
    for kz in range(4):
        oz = (zl - kz) & 3
        years = jnp.zeros((8, LANES), jnp.int32)
        for kx in range(4):
            ox = (x - kx) & 3
            stores = jnp.zeros((8, LANES), jnp.int32)
            for ky in range(4):
                oy = (y - ky) & 3
                at = (ky * 4 + kz) * BLOCK_ROWS + BRAND_ROWS - 1
                moved = lane_gather(spread(tables[kx], at), lane_from)
                stores += jnp.where((lane >> 5) == oy, moved, 0)
                years += jnp.where((lane >> 3) == ox * 4 + oy, moved, 0)
                days += jnp.where((lane >> 1) == oz * 16 + ox * 4 + oy, moved, 0)
            small_ref[pl.ds(oz * 4 + ox, 1), :] = stores[0:1]
        small_ref[pl.ds(16 + oz, 1), :] = years[1:2]
    small_ref[pl.ds(20, 1), :] = days[2:3]

    def filter_block(refs, to, first):
        at = pl.ds(pl.multiple_of(first, 8), 8)
        date, store, product = (ref[at, :] for ref in refs[:3])
        year_lane, year_row = (date >> 3) & 127, date >> 10
        year_word = jnp.zeros_like(date)
        for i in range(4):
            year_word = jnp.where(
                year_row == i, lane_gather(spread(small_ref, 16 + i), year_lane), year_word
            )
        year = (year_word >> ((date & 7) * 4)) & 15
        passed = lane_gather(spread(small_ref, 20), date >> 5) >> (date & 31)
        store_lane, store_row = (store >> 5) & 127, store >> 12
        store_word = jnp.zeros_like(store)
        for i in range(16):
            store_word = jnp.where(
                store_row == i, lane_gather(spread(small_ref, i), store_lane), store_word
            )
        passed &= store_word >> (store & 31)
        here = (product >= 0) & (((product >> 13) & 1) == c)
        at = pl.ds(pl.multiple_of(to + first, 8), 8)
        keep_ref[at, :] = jnp.where(here, passed & 1, 0)
        meta_ref[at, :] = (product & 0xFFFFF) | (year << 20)

    def filter_blocks(turn, _):
        for u in range(4):
            for side, refs in enumerate((own, other)):
                filter_block(refs, side * rows, turn * 32 + u * 8)
        return 0

    lax.fori_loop(0, rows // 32, filter_blocks, 0)

    money_scratch[:rows, :] = own[3][...]
    money_scratch[rows:, :] = other[3][...]
    meta, money, left = packed_up(keep_ref[...], meta_ref[...], money_scratch[...])
    meta_ref[...] = meta
    money_scratch[...] = money
    keep_ref[...] = jnp.zeros_like(keep_ref)

    def search(tables, rows_of, code, lanes, first, number, unroll):
        def step(turn, found):
            found = [list(f) for f in found]
            start = turn * (unroll * BLOCK_ROWS)
            code_now = [v - turn * (unroll * 128) for v in code]
            for u in range(unroll):
                for t in range(len(tables)):
                    for i in range(number):
                        row = spread(tables[t], start + (u * BLOCK_ROWS + first + i))
                        for q in range(rows_of):
                            at = i % 2
                            got = lane_gather(row, lanes[q])
                            found[q][at] = jnp.where(
                                code_now[q] == u * 128 + t * 32 + i, got, found[q][at]
                            )
            return tuple(tuple(f) for f in found)

        zero = jnp.zeros((8, LANES), jnp.int32)
        found = lax.fori_loop(0, 16 // unroll, step, ((zero, zero),) * rows_of)
        return [f[0] | f[1] for f in found]

    def table_of(product):
        return (x - (product >> 16)) & 3

    def code_of(product, row):
        oz, oy = product >> 18, (product >> 14) & 3
        return (((y - oy) & 3) * 4 + ((zl - oz) & 3)) * 128 + row

    def product_blocks(turn, _):
        ats = [pl.ds(pl.multiple_of(turn * 16 + u * 8, 8), 8) for u in range(2)]
        products = [meta_ref[at, :] & 0xFFFFF for at in ats]
        words = search(
            tables,
            2,
            [code_of(p, (p >> 12) & 1) + table_of(p) * 32 for p in products],
            [(p >> 5) & 127 for p in products],
            BRAND_ROWS,
            FLAG_ROWS,
            8,
        )
        for u, (at, product, word) in enumerate(zip(ats, products, words)):
            there = turn * 16 + u * 8 + sub < left
            keep_ref[at, :] = jnp.where(there, (word >> (product & 31)) & 1, 0)
        return 0

    most = jnp.max(left)
    lax.fori_loop(0, (most + 15) // 16, product_blocks, 0)

    def pack_first(rows):
        keep, meta, money = keep_ref[:rows, :], meta_ref[:rows, :] & 0xFFFFFF, money_scratch[:rows, :]
        table = table_of(meta & 0xFFFFF)
        lefts = []
        for t in range(4):
            packed = packed_up(jnp.where(table == t, keep, 0), meta, money)
            metas_ref[t, :rows, :], moneys_ref[t, :rows, :], left = packed
            lefts.append(left)
        return tuple(lefts)

    lefts = lax.cond(most <= 64, lambda: pack_first(64), lambda: pack_first(2 * rows))

    high_row = lax.broadcasted_iota(jnp.int32, (LANES, LANES), 0)

    def hots(t, block):
        at = pl.ds(pl.multiple_of(block * 8, 8), 8)
        meta = metas_ref[t, at, :]
        product, year = meta & 0xFFFFF, (meta >> 20) & 15
        local = product & 16383
        word = (local * 21846) >> 16
        digit = local - word * 3
        code = code_of(product, (word >> 7) - c * SPLIT_ROW)
        (found,) = search([tables[t]], 1, [code], [word & 127], 0, BRAND_ROWS, 16)
        brand = (found >> (digit * 10)) & 1023
        amount = jnp.where(block * 8 + sub < lefts[t], moneys_ref[t, at, :], 0.0)
        high = (brand >> 7) * YEARS + year
        low = brand & 127
        weighted, low_hot = [], []
        for s in range(8):
            weighted.append(
                jnp.where(high_row == high[s : s + 1, :], amount[s : s + 1, :], 0.0).astype(
                    jnp.bfloat16
                )
            )
            low_hot.append((high_row == low[s : s + 1, :]).astype(jnp.float32).astype(jnp.bfloat16))
        return weighted, low_hot

    def summed(pieces):
        weighted = [w for piece in pieces for w in piece[0]]
        low_hot = [h for piece in pieces for h in piece[1]]
        return lax.dot_general(
            jnp.concatenate(weighted, axis=1),
            jnp.concatenate(low_hot, axis=1),
            (((1,), (1,)), ((), ())),
            preferred_element_type=jnp.float32,
        )

    out_ref[...] = summed([hots(t, 0) for t in range(4)])
    for t in range(4):

        def add_block(block, _, t=t):
            out_ref[...] += summed([hots(t, block)])
            return 0

        lax.fori_loop(1, (jnp.max(lefts[t]) + 7) // 8, add_block, 0)


def joined(where, own, other, tables):
    vmem = pl.BlockSpec(memory_space=pltpu.VMEM)
    rows = 2 * own[0].shape[0]
    return pl.pallas_call(
        join_kernel,
        out_shape=jax.ShapeDtypeStruct((LANES, LANES), jnp.float32),
        in_specs=[pl.BlockSpec(memory_space=pltpu.SMEM)] + [vmem] * 12,
        out_specs=vmem,
        scratch_shapes=[
            pltpu.VMEM((24, LANES), jnp.int32),
            pltpu.VMEM((rows, LANES), jnp.int32),
            pltpu.VMEM((rows, LANES), jnp.int32),
            pltpu.VMEM((rows, LANES), jnp.float32),
            pltpu.VMEM((4, rows, LANES), jnp.int32),
            pltpu.VMEM((4, rows, LANES), jnp.float32),
        ],
        cost_estimate=pl.CostEstimate(flops=10**8, bytes_accessed=10**6, transcendentals=0),
        compiler_params=pltpu.CompilerParams(
            vmem_limit_bytes=8 * 2**20
        ),
    )(where, *own, *other, *tables)


def half_kernel(c_ref, packed_ref, out_ref):
    for half in range(2):

        @pl.when(c_ref[0] == half)
        def _(half=half):
            out_ref[:BRAND_ROWS, :] = packed_ref[pl.ds(half * SPLIT_ROW, BRAND_ROWS), :]
            out_ref[BRAND_ROWS:, :] = packed_ref[pl.ds(43 + half * FLAG_ROWS, FLAG_ROWS), :]

    lane = lax.broadcasted_iota(jnp.int32, (1, LANES), 1)
    last = pl.ds(BRAND_ROWS - 1, 1)
    out_ref[last, :] = jnp.where(lane < SMALL_LANE, out_ref[last, :], packed_ref[pl.ds(42, 1), :])


def half_of(c, packed):
    vmem = pl.BlockSpec(memory_space=pltpu.VMEM)
    return pl.pallas_call(
        half_kernel,
        out_shape=jax.ShapeDtypeStruct((BLOCK_ROWS, LANES), jnp.int32),
        in_specs=[pl.BlockSpec(memory_space=pltpu.SMEM), vmem],
        out_specs=vmem,
        compiler_params=pltpu.CompilerParams(vmem_limit_bytes=2**20),
    )(c[None], packed)


def gather_tables(block):
    line = jnp.concatenate(from_behind(block, "z", (1, 2, 3)), axis=0)
    plane = jnp.concatenate(from_behind(line, "y", (1, 3, 2)), axis=0)
    return from_behind(plane, "x", (1, 3, 2))


def four_added(value, axis):
    if axis == "z":
        c, b, a = (swapped(value, axis, bits) for bits in (3, 2, 1))
        return (value + a) + (b + c)
    a, b, c, d = from_behind(value, axis, (1, 3, 2))
    return (a + c) + (b + d)


def sum_everywhere(partial, c):
    def half(at):
        return lax.dynamic_slice_in_dim(partial, at * 64, 64, 0)

    total = half(c) + swapped(half(1 - c), "c", 1)
    for axis in ("x", "y", "z"):
        total = four_added(total, axis)
    total = total + swapped(total, "z", 7)
    return pl.pallas_call(
        lay_kernel,
        out_shape=jax.ShapeDtypeStruct((YEARS, BRANDS), jnp.float32),
        in_specs=[pl.BlockSpec(memory_space=pltpu.SMEM)]
        + [pl.BlockSpec(memory_space=pltpu.VMEM)] * 2,
        out_specs=pl.BlockSpec(memory_space=pltpu.VMEM),
        compiler_params=pltpu.CompilerParams(vmem_limit_bytes=2**20),
    )(c[None], total, swapped(total, "c", 1))


def lay_kernel(c_ref, mine_ref, other_ref, out_ref):
    for side, ref in enumerate((mine_ref, other_ref)):
        for i in range(4):
            at = (c_ref[0] ^ side) * 4 + i
            out_ref[:, pl.ds(pl.multiple_of(at * LANES, LANES), LANES)] = ref[pl.ds(i * 16, 16), :]


def shards(
    date_key,
    store_key,
    product_key,
    revenue,
    row_counts,
    date_years,
    date_flags,
    store_flags,
    product_flags,
    brand_words,
):
    gx, gy = lax.axis_index("gx"), lax.axis_index("gy")
    zl, x, y, c = gx >> 4, (gx >> 2) & 3, gx & 3, gy & 1
    packed = jnp.concatenate(
        [brand_words[: 43 * LANES - 42], store_flags, date_years, date_flags, product_flags]
    ).reshape(47, LANES)
    block = half_of(c, packed)
    live = lax.iota(jnp.int32, product_key.shape[0]) < row_counts[0]
    own = [
        a.reshape(-1, LANES)
        for a in (
            date_key,
            store_key,
            jnp.where(live, product_key, -1),
            revenue.astype(jnp.float32),
        )
    ]
    other = [swapped(a, "c", 1) for a in own]
    tables = gather_tables(block)
    partial = joined(jnp.stack([zl, x, y, c]), own, other, tables)
    return sum_everywhere(partial, c)


def solution(mesh):
    placed = (P(AXES),) * 5 + (P("gx"),) * 5
    return jax.shard_map(shards, mesh=mesh, in_specs=placed, out_specs=P(), check_vma=False)
```

```python
import functools

import jax
import jax.numpy as jnp
from jax import lax
from jax.experimental import pallas as pl
from jax.experimental.pallas import tpu as pltpu
from jax.sharding import PartitionSpec as P

BRANDS = 1024
YEARS = 16
AXES = ("gx", "gy")
LANES = 128
BRAND_ROWS = 22
FLAG_ROWS = 2
BLOCK_ROWS = BRAND_ROWS + FLAG_ROWS
SPLIT_ROW = 21
SMALL_LANE = 86


def place_of(index):
    gx, gy = index // 4, index % 4
    return dict(z=gy // 2 * 4 + gx // 16, x=gx // 4 % 4, y=gx % 4, c=gy % 2)


def index_of(place):
    gx = place["z"] % 4 * 16 + place["x"] * 4 + place["y"]
    return gx * 4 + place["z"] // 4 * 2 + place["c"]


def moved(value, move):
    pairs = []
    for source in range(256):
        place = place_of(source)
        move(place)
        pairs.append((source, index_of(place)))
    return lax.ppermute(value, AXES, pairs)


def swapped(value, axis, bits):
    def move(place):
        place[axis] ^= bits

    return moved(value, move)


def shifted(value, axis, steps):
    def move(place):
        place[axis] = place[axis] // 4 * 4 + (place[axis] + steps) % 4

    return moved(value, move)


def from_behind(value, axis, order):
    far = {steps: shifted(value, axis, steps) for steps in order}
    return [value] + [far[k] for k in (1, 2, 3)]


def lane_gather(rows, lanes):
    return jnp.take_along_axis(rows, lanes, axis=1, mode="promise_in_bounds")


def spread(ref, row):
    return jnp.broadcast_to(ref[pl.ds(row, 1), :], (8, LANES))


def packed_up(keep, meta, money):
    rows = keep.shape[0]
    above = lax.broadcasted_iota(jnp.int32, (rows, rows), 0) > lax.broadcasted_iota(
        jnp.int32, (rows, rows), 1
    )
    dropped = lax.dot_general(
        jnp.where(above, 1.0, 0.0).astype(jnp.bfloat16),
        (1 - keep).astype(jnp.float32).astype(jnp.bfloat16),
        (((1,), (0,)), ((), ())),
        preferred_element_type=jnp.float32,
    ).astype(jnp.int32)
    meta = jnp.where(keep == 1, meta | (dropped << 24), 0)
    for b in range((rows - 1).bit_length()):
        bit = jnp.int32((1 << (24 + b)) if b < 7 else -(2**31))
        coming = pltpu.roll(meta, rows - (1 << b), 0)
        coming_money = pltpu.roll(money, rows - (1 << b), 0)
        take = (coming & bit) != 0
        meta = jnp.where(take, coming, jnp.where((meta & bit) != 0, 0, meta))
        money = jnp.where(take, coming_money, money)
    return meta, money, jnp.sum(keep, axis=0, keepdims=True)


def join_kernel(where_ref, *refs):
    own, other, tables = refs[:4], refs[4:8], refs[8:12]
    out_ref, small_ref, keep_ref, meta_ref, money_scratch = refs[12:17]
    metas_ref, moneys_ref, lefts_ref, mixed_ref = refs[17:]
    zl, x, y, c = (where_ref[i] for i in range(4))
    lane = lax.broadcasted_iota(jnp.int32, (8, LANES), 1)
    sub = lax.broadcasted_iota(jnp.int32, (8, LANES), 0)
    rows = own[0].shape[0]

    lane_from = SMALL_LANE + jnp.where(
        sub == 0, lane & 31, jnp.where(sub == 1, 32 + (lane & 7), 40 + (lane & 1))
    )
    days = jnp.zeros((8, LANES), jnp.int32)
    for kz in range(4):
        oz = (zl - kz) & 3
        years = jnp.zeros((8, LANES), jnp.int32)
        for kx in range(4):
            ox = (x - kx) & 3
            stores = jnp.zeros((8, LANES), jnp.int32)
            for ky in range(4):
                oy = (y - ky) & 3
                at = (ky * 4 + kz) * BLOCK_ROWS + BRAND_ROWS - 1
                moved = lane_gather(spread(tables[kx], at), lane_from)
                stores += jnp.where((lane >> 5) == oy, moved, 0)
                years += jnp.where((lane >> 3) == ox * 4 + oy, moved, 0)
                days += jnp.where((lane >> 1) == oz * 16 + ox * 4 + oy, moved, 0)
            small_ref[pl.ds(oz * 4 + ox, 1), :] = stores[0:1]
        small_ref[pl.ds(16 + oz, 1), :] = years[1:2]
    small_ref[pl.ds(20, 1), :] = days[2:3]

    def filter_block(refs, to, first):
        at = pl.ds(pl.multiple_of(first, 8), 8)
        date, store, product = (ref[at, :] for ref in refs[:3])
        year_lane, year_row = (date >> 3) & 127, date >> 10
        year_word = jnp.zeros_like(date)
        for i in range(4):
            year_word = jnp.where(
                year_row == i, lane_gather(spread(small_ref, 16 + i), year_lane), year_word
            )
        year = (year_word >> ((date & 7) * 4)) & 15
        passed = lane_gather(spread(small_ref, 20), date >> 5) >> (date & 31)
        store_lane, store_row = (store >> 5) & 127, store >> 12
        store_word = jnp.zeros_like(store)
        for i in range(16):
            store_word = jnp.where(
                store_row == i, lane_gather(spread(small_ref, i), store_lane), store_word
            )
        passed &= store_word >> (store & 31)
        here = (product >= 0) & (((product >> 13) & 1) == c)
        at = pl.ds(pl.multiple_of(to + first, 8), 8)
        keep_ref[at, :] = jnp.where(here, passed & 1, 0)
        meta_ref[at, :] = (product & 0xFFFFF) | (year << 20)

    def filter_blocks(turn, _):
        for u in range(4):
            for side, refs in enumerate((own, other)):
                filter_block(refs, side * rows, turn * 32 + u * 8)
        return 0

    lax.fori_loop(0, rows // 32, filter_blocks, 0)

    money_scratch[:rows, :] = own[3][...]
    money_scratch[rows:, :] = other[3][...]
    meta, money, left = packed_up(keep_ref[...], meta_ref[...], money_scratch[...])
    meta_ref[...] = meta
    money_scratch[...] = money
    keep_ref[...] = jnp.zeros_like(keep_ref)

    def search(tables, rows_of, code, lanes, first, number, unroll):
        def step(turn, found):
            found = [list(f) for f in found]
            start = turn * (unroll * BLOCK_ROWS)
            code_now = [v - turn * (unroll * 128) for v in code]
            for u in range(unroll):
                for t in range(len(tables)):
                    for i in range(number):
                        row = spread(tables[t], start + (u * BLOCK_ROWS + first + i))
                        for q in range(rows_of):
                            at = i % 2
                            got = lane_gather(row, lanes[q])
                            found[q][at] = jnp.where(
                                code_now[q] == u * 128 + t * 32 + i, got, found[q][at]
                            )
            return tuple(tuple(f) for f in found)

        zero = jnp.zeros((8, LANES), jnp.int32)
        found = lax.fori_loop(0, 16 // unroll, step, ((zero, zero),) * rows_of)
        return [f[0] | f[1] for f in found]

    def table_of(product):
        return (x - (product >> 16)) & 3

    def code_of(product, row):
        oz, oy = product >> 18, (product >> 14) & 3
        return (((y - oy) & 3) * 4 + ((zl - oz) & 3)) * 128 + row

    def product_blocks(turn, _):
        ats = [pl.ds(pl.multiple_of(turn * 16 + u * 8, 8), 8) for u in range(2)]
        products = [meta_ref[at, :] & 0xFFFFF for at in ats]
        words = search(
            tables,
            2,
            [code_of(p, (p >> 12) & 1) + table_of(p) * 32 for p in products],
            [(p >> 5) & 127 for p in products],
            BRAND_ROWS,
            FLAG_ROWS,
            8,
        )
        for u, (at, product, word) in enumerate(zip(ats, products, words)):
            there = turn * 16 + u * 8 + sub < left
            keep_ref[at, :] = jnp.where(there, (word >> (product & 31)) & 1, 0)
        return 0

    most = jnp.max(left)
    lax.fori_loop(0, (most + 15) // 16, product_blocks, 0)

    def place_in(product):
        owner = ((y - (product >> 14)) & 3) * 4 + ((zl - (product >> 18)) & 3)
        return ((x - (product >> 16)) & 3) * 2 + (owner >> 3), owner & 7

    def pack_group(rows, g):
        meta = meta_ref[:rows, :] & 0xFFFFFF
        mine = place_in(meta & 0xFFFFF)[0] == g
        keep = jnp.where(mine, keep_ref[:rows, :], 0)
        meta, money, left = packed_up(keep, meta, money_scratch[:rows, :])
        metas_ref[pl.ds(g, rows, stride=8), :] = meta
        moneys_ref[pl.ds(g, rows, stride=8), :] = money
        lefts_ref[pl.ds(g, 1), :] = left

    @pl.when(most <= 64)
    def _():
        for g in range(8):
            pack_group(64, g)

    @pl.when(most > 64)
    def _():
        def pack_next(g, _):
            pack_group(2 * rows, g)
            return 0

        lax.fori_loop(0, 8, pack_next, 0)

    half_rows = 8 * BLOCK_ROWS
    for g in range(8):
        mixed_ref[pl.ds(g, half_rows, stride=8), :] = tables[g // 2][
            pl.ds(g % 2 * half_rows, half_rows), :
        ]

    lefts = lefts_ref[...]
    sixteen = lax.broadcasted_iota(jnp.int32, (16, LANES), 0)
    numbers = [(sixteen + 16 * k).astype(jnp.float32).astype(jnp.bfloat16) for k in range(8)]

    def wide(values, s):
        row = jnp.broadcast_to(values[s : s + 1, :].astype(jnp.float32), (16, LANES))
        return row.astype(jnp.bfloat16)

    out_ref[...] = jnp.zeros_like(out_ref)

    def add_blocks(turn, _):
        ats, years, digits, codes, lanes = [], [], [], [], []
        for u in range(4):
            at = pl.ds(pl.multiple_of(turn * 32 + u * 8, 8), 8)
            meta = metas_ref[at, :]
            product = meta & 0xFFFFF
            local = product & 16383
            word = (local * 21846) >> 16
            ats.append(at)
            years.append((meta >> 20) & 15)
            digits.append(local - word * 3)
            codes.append(place_in(product)[1] * 32 + (word >> 7) - c * SPLIT_ROW)
            lanes.append(word & 127)

        def step(part, found):
            found = [list(f) for f in found]
            for q in range(4):
                code = codes[q] - part * 128
                for u in range(4):
                    for i in range(BRAND_ROWS):
                        start = part * (4 * BLOCK_ROWS * 8) + (u * BLOCK_ROWS + i) * 8
                        row = mixed_ref[pl.ds(pl.multiple_of(start, 8), 8), :]
                        got = lane_gather(row, lanes[q])
                        found[q][i % 2] = jnp.where(code == u * 32 + i, got, found[q][i % 2])
            return tuple(tuple(f) for f in found)

        zero = jnp.zeros((8, LANES), jnp.int32)
        found = lax.fori_loop(0, 2, step, ((zero, zero),) * 4)
        weighted, low_hot = [], []
        for u in range(4):
            brand = ((found[u][0] | found[u][1]) >> (digits[u] * 10)) & 1023
            amount = jnp.where(turn * 4 + u < lefts, moneys_ref[ats[u], :], 0.0)
            high = (brand >> 7) * YEARS + years[u]
            low = brand & 127
            one, none = jnp.ones((16, LANES), jnp.bfloat16), jnp.zeros((16, LANES), jnp.bfloat16)
            for s in range(8):
                high_now, low_now, amount_now = (wide(v, s) for v in (high, low, amount))
                weighted.append(
                    jnp.concatenate(
                        [jnp.where(n == high_now, amount_now, none) for n in numbers], axis=0
                    )
                )
                low_hot.append(
                    jnp.concatenate([jnp.where(n == low_now, one, none) for n in numbers], axis=0)
                )
        out_ref[...] += lax.dot_general(
            jnp.concatenate(weighted, axis=1),
            jnp.concatenate(low_hot, axis=1),
            (((1,), (1,)), ((), ())),
            preferred_element_type=jnp.float32,
        )
        return 0

    lax.fori_loop(0, (jnp.max(lefts) + 3) // 4, add_blocks, 0)


def joined(where, own, other, tables):
    vmem = pl.BlockSpec(memory_space=pltpu.VMEM)
    rows = 2 * own[0].shape[0]
    return pl.pallas_call(
        join_kernel,
        out_shape=jax.ShapeDtypeStruct((LANES, LANES), jnp.float32),
        in_specs=[pl.BlockSpec(memory_space=pltpu.SMEM)] + [vmem] * 12,
        out_specs=vmem,
        scratch_shapes=[
            pltpu.VMEM((24, LANES), jnp.int32),
            pltpu.VMEM((rows, LANES), jnp.int32),
            pltpu.VMEM((rows, LANES), jnp.int32),
            pltpu.VMEM((rows, LANES), jnp.float32),
            pltpu.VMEM((8 * rows, LANES), jnp.int32),
            pltpu.VMEM((8 * rows, LANES), jnp.float32),
            pltpu.VMEM((8, LANES), jnp.int32),
            pltpu.VMEM((64 * BLOCK_ROWS, LANES), jnp.int32),
        ],
        cost_estimate=pl.CostEstimate(flops=10**8, bytes_accessed=10**6, transcendentals=0),
        compiler_params=pltpu.CompilerParams(
            vmem_limit_bytes=8 * 2**20
        ),
    )(where, *own, *other, *tables)


def half_kernel(c_ref, packed_ref, out_ref):
    for half in range(2):

        @pl.when(c_ref[0] == half)
        def _(half=half):
            out_ref[:BRAND_ROWS, :] = packed_ref[pl.ds(half * SPLIT_ROW, BRAND_ROWS), :]
            out_ref[BRAND_ROWS:, :] = packed_ref[pl.ds(43 + half * FLAG_ROWS, FLAG_ROWS), :]

    lane = lax.broadcasted_iota(jnp.int32, (1, LANES), 1)
    last = pl.ds(BRAND_ROWS - 1, 1)
    out_ref[last, :] = jnp.where(lane < SMALL_LANE, out_ref[last, :], packed_ref[pl.ds(42, 1), :])


def half_of(c, packed):
    vmem = pl.BlockSpec(memory_space=pltpu.VMEM)
    return pl.pallas_call(
        half_kernel,
        out_shape=jax.ShapeDtypeStruct((BLOCK_ROWS, LANES), jnp.int32),
        in_specs=[pl.BlockSpec(memory_space=pltpu.SMEM), vmem],
        out_specs=vmem,
        compiler_params=pltpu.CompilerParams(vmem_limit_bytes=2**20),
    )(c[None], packed)


def gather_tables(block):
    line = jnp.concatenate(from_behind(block, "z", (1, 2, 3)), axis=0)
    plane = jnp.concatenate(from_behind(line, "y", (1, 3, 2)), axis=0)
    return from_behind(plane, "x", (1, 3, 2))


def four_added(value, axis):
    if axis == "z":
        c, b, a = (swapped(value, axis, bits) for bits in (3, 2, 1))
        return (value + a) + (b + c)
    a, b, c, d = from_behind(value, axis, (1, 3, 2))
    return (a + c) + (b + d)


def sum_everywhere(partial, c):
    def half(at):
        return lax.dynamic_slice_in_dim(partial, at * 64, 64, 0)

    total = half(c) + swapped(half(1 - c), "c", 1)
    for axis in ("x", "y", "z"):
        total = four_added(total, axis)
    total = total + swapped(total, "z", 7)
    return pl.pallas_call(
        lay_kernel,
        out_shape=jax.ShapeDtypeStruct((YEARS, BRANDS), jnp.float32),
        in_specs=[pl.BlockSpec(memory_space=pltpu.SMEM)]
        + [pl.BlockSpec(memory_space=pltpu.VMEM)] * 2,
        out_specs=pl.BlockSpec(memory_space=pltpu.VMEM),
        compiler_params=pltpu.CompilerParams(vmem_limit_bytes=2**20),
    )(c[None], total, swapped(total, "c", 1))


def lay_kernel(c_ref, mine_ref, other_ref, out_ref):
    for side, ref in enumerate((mine_ref, other_ref)):
        for i in range(4):
            at = (c_ref[0] ^ side) * 4 + i
            out_ref[:, pl.ds(pl.multiple_of(at * LANES, LANES), LANES)] = ref[pl.ds(i * 16, 16), :]


def shards(
    date_key,
    store_key,
    product_key,
    revenue,
    row_counts,
    date_years,
    date_flags,
    store_flags,
    product_flags,
    brand_words,
):
    gx, gy = lax.axis_index("gx"), lax.axis_index("gy")
    zl, x, y, c = gx >> 4, (gx >> 2) & 3, gx & 3, gy & 1
    packed = jnp.concatenate(
        [brand_words[: 43 * LANES - 42], store_flags, date_years, date_flags, product_flags]
    ).reshape(47, LANES)
    block = half_of(c, packed)
    live = lax.iota(jnp.int32, product_key.shape[0]) < row_counts[0]
    own = [
        a.reshape(-1, LANES)
        for a in (
            date_key,
            store_key,
            jnp.where(live, product_key, -1),
            revenue.astype(jnp.float32),
        )
    ]
    other = [swapped(a, "c", 1) for a in own]
    tables = gather_tables(block)
    partial = joined(jnp.stack([zl, x, y, c]), own, other, tables)
    return sum_everywhere(partial, c)


def solution(mesh):
    placed = (P(AXES),) * 5 + (P("gx"),) * 5
    return jax.shard_map(shards, mesh=mesh, in_specs=placed, out_specs=P(), check_vma=False)
```

```python
import functools

import jax
import jax.numpy as jnp
from jax import lax
from jax.experimental import pallas as pl
from jax.experimental.pallas import tpu as pltpu
from jax.sharding import PartitionSpec as P

BRANDS = 1024
YEARS = 16
AXES = ("gx", "gy")
LANES = 128
BRAND_ROWS = 22
FLAG_ROWS = 2
BLOCK_ROWS = BRAND_ROWS + FLAG_ROWS
SPLIT_ROW = 21
FEW_ROWS = 48
SMALL_LANE = 86


def place_of(index):
    gx, gy = index // 4, index % 4
    return dict(z=gy // 2 * 4 + gx // 16, x=gx // 4 % 4, y=gx % 4, c=gy % 2)


def index_of(place):
    gx = place["z"] % 4 * 16 + place["x"] * 4 + place["y"]
    return gx * 4 + place["z"] // 4 * 2 + place["c"]


def moved(value, move):
    pairs = []
    for source in range(256):
        place = place_of(source)
        move(place)
        pairs.append((source, index_of(place)))
    return lax.ppermute(value, AXES, pairs)


def swapped(value, axis, bits):
    def move(place):
        place[axis] ^= bits

    return moved(value, move)


def shifted(value, axis, steps):
    def move(place):
        place[axis] = place[axis] // 4 * 4 + (place[axis] + steps) % 4

    return moved(value, move)


def from_behind(value, axis, order):
    far = {steps: shifted(value, axis, steps) for steps in order}
    return [value] + [far[k] for k in (1, 2, 3)]


def lane_gather(rows, lanes):
    return jnp.take_along_axis(rows, lanes, axis=1, mode="promise_in_bounds")


def spread(ref, row):
    return jnp.broadcast_to(ref[pl.ds(row, 1), :], (8, LANES))


def packed_up(keep, meta, money):
    rows = keep.shape[0]
    above = lax.broadcasted_iota(jnp.int32, (rows, rows), 0) > lax.broadcasted_iota(
        jnp.int32, (rows, rows), 1
    )
    dropped = lax.dot_general(
        jnp.where(above, 1.0, 0.0).astype(jnp.bfloat16),
        (1 - keep).astype(jnp.float32).astype(jnp.bfloat16),
        (((1,), (0,)), ((), ())),
        preferred_element_type=jnp.float32,
    ).astype(jnp.int32)
    meta = jnp.where(keep == 1, meta | (dropped << 24), 0)
    for b in range((rows - 1).bit_length()):
        bit = jnp.int32((1 << (24 + b)) if b < 7 else -(2**31))
        coming = pltpu.roll(meta, rows - (1 << b), 0)
        coming_money = pltpu.roll(money, rows - (1 << b), 0)
        take = (coming & bit) != 0
        meta = jnp.where(take, coming, jnp.where((meta & bit) != 0, 0, meta))
        money = jnp.where(take, coming_money, money)
    return meta, money, jnp.sum(keep, axis=0, keepdims=True)


def join_kernel(where_ref, *refs):
    own, other, tables = refs[:4], refs[4:8], refs[8:12]
    out_ref, small_ref, keep_ref, meta_ref, money_scratch = refs[12:17]
    metas_ref, moneys_ref, lefts_ref, mixed_ref = refs[17:]
    zl, x, y, c = (where_ref[i] for i in range(4))
    lane = lax.broadcasted_iota(jnp.int32, (8, LANES), 1)
    sub = lax.broadcasted_iota(jnp.int32, (8, LANES), 0)
    rows = own[0].shape[0]

    lane_from = SMALL_LANE + jnp.where(
        sub == 0, lane & 31, jnp.where(sub == 1, 32 + (lane & 7), 40 + (lane & 1))
    )
    days = jnp.zeros((8, LANES), jnp.int32)
    for kz in range(4):
        oz = (zl - kz) & 3
        years = jnp.zeros((8, LANES), jnp.int32)
        for kx in range(4):
            ox = (x - kx) & 3
            stores = jnp.zeros((8, LANES), jnp.int32)
            for ky in range(4):
                oy = (y - ky) & 3
                at = (ky * 4 + kz) * BLOCK_ROWS + BRAND_ROWS - 1
                moved = lane_gather(spread(tables[kx], at), lane_from)
                stores += jnp.where((lane >> 5) == oy, moved, 0)
                years += jnp.where((lane >> 3) == ox * 4 + oy, moved, 0)
                days += jnp.where((lane >> 1) == oz * 16 + ox * 4 + oy, moved, 0)
            small_ref[pl.ds(oz * 4 + ox, 1), :] = stores[0:1]
        small_ref[pl.ds(16 + oz, 1), :] = years[1:2]
    small_ref[pl.ds(20, 1), :] = days[2:3]

    def filter_block(refs, to, first):
        at = pl.ds(pl.multiple_of(first, 8), 8)
        date, store, product = (ref[at, :] for ref in refs[:3])
        year_lane, year_row = (date >> 3) & 127, date >> 10
        year_word = jnp.zeros_like(date)
        for i in range(4):
            year_word = jnp.where(
                year_row == i, lane_gather(spread(small_ref, 16 + i), year_lane), year_word
            )
        year = (year_word >> ((date & 7) * 4)) & 15
        passed = lane_gather(spread(small_ref, 20), date >> 5) >> (date & 31)
        store_lane, store_row = (store >> 5) & 127, store >> 12
        store_word = jnp.zeros_like(store)
        for i in range(16):
            store_word = jnp.where(
                store_row == i, lane_gather(spread(small_ref, i), store_lane), store_word
            )
        passed &= store_word >> (store & 31)
        here = (product >= 0) & (((product >> 13) & 1) == c)
        at = pl.ds(pl.multiple_of(to + first, 8), 8)
        keep_ref[at, :] = jnp.where(here, passed & 1, 0)
        meta_ref[at, :] = (product & 0xFFFFF) | (year << 20)

    def filter_blocks(turn, _):
        for u in range(4):
            for side, refs in enumerate((own, other)):
                filter_block(refs, side * rows, turn * 32 + u * 8)
        return 0

    lax.fori_loop(0, rows // 32, filter_blocks, 0)

    money_scratch[:rows, :] = own[3][...]
    money_scratch[rows:, :] = other[3][...]
    meta, money, left = packed_up(keep_ref[...], meta_ref[...], money_scratch[...])
    meta_ref[...] = meta
    money_scratch[...] = money
    keep_ref[...] = jnp.zeros_like(keep_ref)

    def search(tables, rows_of, code, lanes, first, number, unroll):
        def step(turn, found):
            found = [list(f) for f in found]
            start = turn * (unroll * BLOCK_ROWS)
            code_now = [v - turn * (unroll * 128) for v in code]
            for u in range(unroll):
                for t in range(len(tables)):
                    for i in range(number):
                        row = spread(tables[t], start + (u * BLOCK_ROWS + first + i))
                        for q in range(rows_of):
                            at = i % 2
                            got = lane_gather(row, lanes[q])
                            found[q][at] = jnp.where(
                                code_now[q] == u * 128 + t * 32 + i, got, found[q][at]
                            )
            return tuple(tuple(f) for f in found)

        zero = jnp.zeros((8, LANES), jnp.int32)
        found = lax.fori_loop(0, 16 // unroll, step, ((zero, zero),) * rows_of)
        return [f[0] | f[1] for f in found]

    def table_of(product):
        return (x - (product >> 16)) & 3

    def code_of(product, row):
        oz, oy = product >> 18, (product >> 14) & 3
        return (((y - oy) & 3) * 4 + ((zl - oz) & 3)) * 128 + row

    def product_blocks(turn, _):
        ats = [pl.ds(pl.multiple_of(turn * 16 + u * 8, 8), 8) for u in range(2)]
        products = [meta_ref[at, :] & 0xFFFFF for at in ats]
        words = search(
            tables,
            2,
            [code_of(p, (p >> 12) & 1) + table_of(p) * 32 for p in products],
            [(p >> 5) & 127 for p in products],
            BRAND_ROWS,
            FLAG_ROWS,
            16,
        )
        for u, (at, product, word) in enumerate(zip(ats, products, words)):
            there = turn * 16 + u * 8 + sub < left
            keep_ref[at, :] = jnp.where(there, (word >> (product & 31)) & 1, 0)
        return 0

    most = jnp.max(left)
    lax.fori_loop(0, (most + 15) // 16, product_blocks, 0)

    def place_in(product):
        owner = ((y - (product >> 14)) & 3) * 4 + ((zl - (product >> 18)) & 3)
        return ((x - (product >> 16)) & 3) * 2 + (owner >> 3), owner & 7

    def pack_group(rows, g):
        meta = meta_ref[:rows, :] & 0xFFFFFF
        mine = place_in(meta & 0xFFFFF)[0] == g
        keep = jnp.where(mine, keep_ref[:rows, :], 0)
        meta, money, left = packed_up(keep, meta, money_scratch[:rows, :])
        metas_ref[pl.ds(g, rows, stride=8), :] = meta
        moneys_ref[pl.ds(g, rows, stride=8), :] = money
        lefts_ref[pl.ds(g, 1), :] = left

    @pl.when(most <= FEW_ROWS)
    def _():
        for g in range(8):
            pack_group(FEW_ROWS, g)

    @pl.when(most > FEW_ROWS)
    def _():
        def pack_next(g, _):
            pack_group(2 * rows, g)
            return 0

        lax.fori_loop(0, 8, pack_next, 0)

    half_rows = 8 * BLOCK_ROWS
    for g in range(8):
        mixed_ref[pl.ds(g, half_rows, stride=8), :] = tables[g // 2][
            pl.ds(g % 2 * half_rows, half_rows), :
        ]

    lefts = lefts_ref[...]
    sixteen = lax.broadcasted_iota(jnp.int32, (16, LANES), 0)
    numbers = [(sixteen + 16 * k).astype(jnp.float32).astype(jnp.bfloat16) for k in range(8)]

    def wide(values, s):
        row = jnp.broadcast_to(values[s : s + 1, :].astype(jnp.float32), (16, LANES))
        return row.astype(jnp.bfloat16)

    out_ref[...] = jnp.zeros_like(out_ref)

    def add_blocks(turn, _):
        ats, years, digits, codes, lanes = [], [], [], [], []
        for u in range(4):
            at = pl.ds(pl.multiple_of(turn * 32 + u * 8, 8), 8)
            meta = metas_ref[at, :]
            product = meta & 0xFFFFF
            local = product & 16383
            word = (local * 21846) >> 16
            ats.append(at)
            years.append((meta >> 20) & 15)
            digits.append(local - word * 3)
            codes.append(place_in(product)[1] * 32 + (word >> 7) - c * SPLIT_ROW)
            lanes.append(word & 127)

        def step(part, found):
            found = [list(f) for f in found]
            for q in range(4):
                code = codes[q] - part * 128
                for u in range(4):
                    for i in range(BRAND_ROWS):
                        start = part * (4 * BLOCK_ROWS * 8) + (u * BLOCK_ROWS + i) * 8
                        row = mixed_ref[pl.ds(pl.multiple_of(start, 8), 8), :]
                        got = lane_gather(row, lanes[q])
                        found[q][i % 2] = jnp.where(code == u * 32 + i, got, found[q][i % 2])
            return tuple(tuple(f) for f in found)

        zero = jnp.zeros((8, LANES), jnp.int32)
        found = lax.fori_loop(0, 2, step, ((zero, zero),) * 4)
        weighted, low_hot = [], []
        for u in range(4):
            brand = ((found[u][0] | found[u][1]) >> (digits[u] * 10)) & 1023
            amount = jnp.where(turn * 4 + u < lefts, moneys_ref[ats[u], :], 0.0)
            high = (brand >> 7) * YEARS + years[u]
            low = brand & 127
            one, none = jnp.ones((16, LANES), jnp.bfloat16), jnp.zeros((16, LANES), jnp.bfloat16)
            for s in range(8):
                high_now, low_now, amount_now = (wide(v, s) for v in (high, low, amount))
                weighted.append(
                    jnp.concatenate(
                        [jnp.where(n == high_now, amount_now, none) for n in numbers], axis=0
                    )
                )
                low_hot.append(
                    jnp.concatenate([jnp.where(n == low_now, one, none) for n in numbers], axis=0)
                )
        out_ref[...] += lax.dot_general(
            jnp.concatenate(weighted, axis=1),
            jnp.concatenate(low_hot, axis=1),
            (((1,), (1,)), ((), ())),
            preferred_element_type=jnp.float32,
        )
        return 0

    lax.fori_loop(0, (jnp.max(lefts) + 3) // 4, add_blocks, 0)


def joined(where, own, other, tables):
    vmem = pl.BlockSpec(memory_space=pltpu.VMEM)
    rows = 2 * own[0].shape[0]
    return pl.pallas_call(
        join_kernel,
        out_shape=jax.ShapeDtypeStruct((LANES, LANES), jnp.float32),
        in_specs=[pl.BlockSpec(memory_space=pltpu.SMEM)] + [vmem] * 12,
        out_specs=vmem,
        scratch_shapes=[
            pltpu.VMEM((24, LANES), jnp.int32),
            pltpu.VMEM((rows, LANES), jnp.int32),
            pltpu.VMEM((rows, LANES), jnp.int32),
            pltpu.VMEM((rows, LANES), jnp.float32),
            pltpu.VMEM((8 * rows, LANES), jnp.int32),
            pltpu.VMEM((8 * rows, LANES), jnp.float32),
            pltpu.VMEM((8, LANES), jnp.int32),
            pltpu.VMEM((64 * BLOCK_ROWS, LANES), jnp.int32),
        ],
        cost_estimate=pl.CostEstimate(flops=10**8, bytes_accessed=10**6, transcendentals=0),
        compiler_params=pltpu.CompilerParams(
            vmem_limit_bytes=8 * 2**20
        ),
    )(where, *own, *other, *tables)


def half_kernel(c_ref, packed_ref, out_ref):
    for half in range(2):

        @pl.when(c_ref[0] == half)
        def _(half=half):
            out_ref[:BRAND_ROWS, :] = packed_ref[pl.ds(half * SPLIT_ROW, BRAND_ROWS), :]
            out_ref[BRAND_ROWS:, :] = packed_ref[pl.ds(43 + half * FLAG_ROWS, FLAG_ROWS), :]

    lane = lax.broadcasted_iota(jnp.int32, (1, LANES), 1)
    last = pl.ds(BRAND_ROWS - 1, 1)
    out_ref[last, :] = jnp.where(lane < SMALL_LANE, out_ref[last, :], packed_ref[pl.ds(42, 1), :])


def half_of(c, packed):
    vmem = pl.BlockSpec(memory_space=pltpu.VMEM)
    return pl.pallas_call(
        half_kernel,
        out_shape=jax.ShapeDtypeStruct((BLOCK_ROWS, LANES), jnp.int32),
        in_specs=[pl.BlockSpec(memory_space=pltpu.SMEM), vmem],
        out_specs=vmem,
        compiler_params=pltpu.CompilerParams(vmem_limit_bytes=2**20),
    )(c[None], packed)


def gather_tables(block):
    line = jnp.concatenate(from_behind(block, "z", (1, 2, 3)), axis=0)
    plane = jnp.concatenate(from_behind(line, "y", (1, 3, 2)), axis=0)
    return from_behind(plane, "x", (1, 3, 2))


def four_added(value, axis):
    if axis == "z":
        c, b, a = (swapped(value, axis, bits) for bits in (3, 2, 1))
        return (value + a) + (b + c)
    a, b, c, d = from_behind(value, axis, (1, 3, 2))
    return (a + c) + (b + d)


def sum_everywhere(partial, c):
    def half(at):
        return lax.dynamic_slice_in_dim(partial, at * 64, 64, 0)

    total = half(c) + swapped(half(1 - c), "c", 1)
    for axis in ("x", "y", "z"):
        total = four_added(total, axis)
    total = total + swapped(total, "z", 7)
    return pl.pallas_call(
        lay_kernel,
        out_shape=jax.ShapeDtypeStruct((YEARS, BRANDS), jnp.float32),
        in_specs=[pl.BlockSpec(memory_space=pltpu.SMEM)]
        + [pl.BlockSpec(memory_space=pltpu.VMEM)] * 2,
        out_specs=pl.BlockSpec(memory_space=pltpu.VMEM),
        compiler_params=pltpu.CompilerParams(vmem_limit_bytes=2**20),
    )(c[None], total, swapped(total, "c", 1))


def lay_kernel(c_ref, mine_ref, other_ref, out_ref):
    for side, ref in enumerate((mine_ref, other_ref)):
        for i in range(4):
            at = (c_ref[0] ^ side) * 4 + i
            out_ref[:, pl.ds(pl.multiple_of(at * LANES, LANES), LANES)] = ref[pl.ds(i * 16, 16), :]


def shards(
    date_key,
    store_key,
    product_key,
    revenue,
    row_counts,
    date_years,
    date_flags,
    store_flags,
    product_flags,
    brand_words,
):
    gx, gy = lax.axis_index("gx"), lax.axis_index("gy")
    zl, x, y, c = gx >> 4, (gx >> 2) & 3, gx & 3, gy & 1
    packed = jnp.concatenate(
        [brand_words[: 43 * LANES - 42], store_flags, date_years, date_flags, product_flags]
    ).reshape(47, LANES)
    block = half_of(c, packed)
    live = lax.iota(jnp.int32, product_key.shape[0]) < row_counts[0]
    own = [
        a.reshape(-1, LANES)
        for a in (
            date_key,
            store_key,
            jnp.where(live, product_key, -1),
            revenue.astype(jnp.float32),
        )
    ]
    other = [swapped(a, "c", 1) for a in own]
    tables = gather_tables(block)
    partial = joined(jnp.stack([zl, x, y, c]), own, other, tables)
    return sum_everywhere(partial, c)


def solution(mesh):
    placed = (P(AXES),) * 5 + (P("gx"),) * 5
    return jax.shard_map(shards, mesh=mesh, in_specs=placed, out_specs=P(), check_vma=False)
```

```python
import functools

import jax
import jax.numpy as jnp
from jax import lax
from jax.experimental import pallas as pl
from jax.experimental.pallas import tpu as pltpu
from jax.sharding import PartitionSpec as P

BRANDS = 1024
YEARS = 16
AXES = ("gx", "gy")
LANES = 128
BRAND_ROWS = 22
FLAG_ROWS = 2
BLOCK_ROWS = BRAND_ROWS + FLAG_ROWS
SPLIT_ROW = 21
FEW_ROWS = 48
SMALL_LANE = 86


def place_of(index):
    gx, gy = index // 4, index % 4
    return dict(z=gy // 2 * 4 + gx // 16, x=gx // 4 % 4, y=gx % 4, c=gy % 2)


def index_of(place):
    gx = place["z"] % 4 * 16 + place["x"] * 4 + place["y"]
    return gx * 4 + place["z"] // 4 * 2 + place["c"]


def moved(value, move):
    pairs = []
    for source in range(256):
        place = place_of(source)
        move(place)
        pairs.append((source, index_of(place)))
    return lax.ppermute(value, AXES, pairs)


def swapped(value, axis, bits):
    def move(place):
        place[axis] ^= bits

    return moved(value, move)


def shifted(value, axis, steps):
    def move(place):
        place[axis] = place[axis] // 4 * 4 + (place[axis] + steps) % 4

    return moved(value, move)


def from_behind(value, axis, order):
    far = {steps: shifted(value, axis, steps) for steps in order}
    return [value] + [far[k] for k in (1, 2, 3)]


def lane_gather(rows, lanes):
    return jnp.take_along_axis(rows, lanes, axis=1, mode="promise_in_bounds")


def spread(ref, row):
    return jnp.broadcast_to(ref[pl.ds(row, 1), :], (8, LANES))


def packed_up(keep, meta, money):
    rows = keep.shape[0]
    above = lax.broadcasted_iota(jnp.int32, (rows, rows), 0) > lax.broadcasted_iota(
        jnp.int32, (rows, rows), 1
    )
    dropped = lax.dot_general(
        jnp.where(above, 1.0, 0.0).astype(jnp.bfloat16),
        (1 - keep).astype(jnp.float32).astype(jnp.bfloat16),
        (((1,), (0,)), ((), ())),
        preferred_element_type=jnp.float32,
    ).astype(jnp.int32)
    meta = jnp.where(keep == 1, meta | (dropped << 24), 0)
    for b in range((rows - 1).bit_length()):
        bit = jnp.int32((1 << (24 + b)) if b < 7 else -(2**31))
        coming = pltpu.roll(meta, rows - (1 << b), 0)
        coming_money = pltpu.roll(money, rows - (1 << b), 0)
        take = (coming & bit) != 0
        meta = jnp.where(take, coming, jnp.where((meta & bit) != 0, 0, meta))
        money = jnp.where(take, coming_money, money)
    return meta, money, jnp.sum(keep, axis=0, keepdims=True)


def join_kernel(where_ref, *refs):
    own, other, tables = refs[:4], refs[4:8], refs[8:12]
    out_ref, small_ref, keep_ref, meta_ref, money_scratch = refs[12:17]
    metas_ref, moneys_ref, lefts_ref, mixed_ref = refs[17:]
    zl, x, y, c = (where_ref[i] for i in range(4))
    lane = lax.broadcasted_iota(jnp.int32, (8, LANES), 1)
    sub = lax.broadcasted_iota(jnp.int32, (8, LANES), 0)
    rows = own[0].shape[0]

    half_rows = 8 * BLOCK_ROWS
    for g in range(8):
        mixed_ref[pl.ds(g, half_rows, stride=8), :] = tables[g // 2][
            pl.ds(g % 2 * half_rows, half_rows), :
        ]

    lane_from = SMALL_LANE + jnp.where(
        sub == 0, lane & 31, jnp.where(sub == 1, 32 + (lane & 7), 40 + (lane & 1))
    )
    days = jnp.zeros((8, LANES), jnp.int32)
    for kz in range(4):
        oz = (zl - kz) & 3
        years = jnp.zeros((8, LANES), jnp.int32)
        for kx in range(4):
            ox = (x - kx) & 3
            stores = jnp.zeros((8, LANES), jnp.int32)
            for ky in range(4):
                oy = (y - ky) & 3
                at = (ky * 4 + kz) * BLOCK_ROWS + BRAND_ROWS - 1
                moved = lane_gather(spread(tables[kx], at), lane_from)
                stores += jnp.where((lane >> 5) == oy, moved, 0)
                years += jnp.where((lane >> 3) == ox * 4 + oy, moved, 0)
                days += jnp.where((lane >> 1) == oz * 16 + ox * 4 + oy, moved, 0)
            small_ref[pl.ds(oz * 4 + ox, 1), :] = stores[0:1]
        small_ref[pl.ds(16 + oz, 1), :] = years[1:2]
    small_ref[pl.ds(20, 1), :] = days[2:3]

    def filter_block(refs, to, first):
        at = pl.ds(pl.multiple_of(first, 8), 8)
        date, store, product = (ref[at, :] for ref in refs[:3])
        year_lane, year_row = (date >> 3) & 127, date >> 10
        year_word = jnp.zeros_like(date)
        for i in range(4):
            year_word = jnp.where(
                year_row == i, lane_gather(spread(small_ref, 16 + i), year_lane), year_word
            )
        year = (year_word >> ((date & 7) * 4)) & 15
        passed = lane_gather(spread(small_ref, 20), date >> 5) >> (date & 31)
        store_lane, store_row = (store >> 5) & 127, store >> 12
        store_word = jnp.zeros_like(store)
        for i in range(16):
            store_word = jnp.where(
                store_row == i, lane_gather(spread(small_ref, i), store_lane), store_word
            )
        passed &= store_word >> (store & 31)
        here = (product >= 0) & (((product >> 13) & 1) == c)
        at = pl.ds(pl.multiple_of(to + first, 8), 8)
        keep_ref[at, :] = jnp.where(here, passed & 1, 0)
        meta_ref[at, :] = (product & 0xFFFFF) | (year << 20)

    def filter_blocks(turn, _):
        for u in range(4):
            for side, refs in enumerate((own, other)):
                filter_block(refs, side * rows, turn * 32 + u * 8)
        return 0

    lax.fori_loop(0, rows // 32, filter_blocks, 0)

    money_scratch[:rows, :] = own[3][...]
    money_scratch[rows:, :] = other[3][...]
    meta, money, left = packed_up(keep_ref[...], meta_ref[...], money_scratch[...])
    meta_ref[...] = meta
    money_scratch[...] = money
    keep_ref[...] = jnp.zeros_like(keep_ref)

    def search(tables, rows_of, code, lanes, first, number, unroll):
        def step(turn, found):
            found = [list(f) for f in found]
            start = turn * (unroll * BLOCK_ROWS)
            code_now = [v - turn * (unroll * 128) for v in code]
            for u in range(unroll):
                for t in range(len(tables)):
                    for i in range(number):
                        row = spread(tables[t], start + (u * BLOCK_ROWS + first + i))
                        for q in range(rows_of):
                            at = i % 2
                            got = lane_gather(row, lanes[q])
                            found[q][at] = jnp.where(
                                code_now[q] == u * 128 + t * 32 + i, got, found[q][at]
                            )
            return tuple(tuple(f) for f in found)

        zero = jnp.zeros((8, LANES), jnp.int32)
        found = lax.fori_loop(0, 16 // unroll, step, ((zero, zero),) * rows_of)
        return [f[0] | f[1] for f in found]

    def table_of(product):
        return (x - (product >> 16)) & 3

    def code_of(product, row):
        oz, oy = product >> 18, (product >> 14) & 3
        return (((y - oy) & 3) * 4 + ((zl - oz) & 3)) * 128 + row

    def product_blocks(turn, _):
        ats = [pl.ds(pl.multiple_of(turn * 16 + u * 8, 8), 8) for u in range(2)]
        products = [meta_ref[at, :] & 0xFFFFF for at in ats]
        words = search(
            tables,
            2,
            [code_of(p, (p >> 12) & 1) + table_of(p) * 32 for p in products],
            [(p >> 5) & 127 for p in products],
            BRAND_ROWS,
            FLAG_ROWS,
            16,
        )
        for u, (at, product, word) in enumerate(zip(ats, products, words)):
            there = turn * 16 + u * 8 + sub < left
            keep_ref[at, :] = jnp.where(there, (word >> (product & 31)) & 1, 0)
        return 0

    most = jnp.max(left)
    lax.fori_loop(0, (most + 15) // 16, product_blocks, 0)

    def place_in(product):
        owner = ((y - (product >> 14)) & 3) * 4 + ((zl - (product >> 18)) & 3)
        return ((x - (product >> 16)) & 3) * 2 + (owner >> 3), owner & 7

    def pack_group(rows, g):
        meta = meta_ref[:rows, :] & 0xFFFFFF
        mine = place_in(meta & 0xFFFFF)[0] == g
        keep = jnp.where(mine, keep_ref[:rows, :], 0)
        meta, money, left = packed_up(keep, meta, money_scratch[:rows, :])
        metas_ref[pl.ds(g, rows, stride=8), :] = meta
        moneys_ref[pl.ds(g, rows, stride=8), :] = money
        lefts_ref[pl.ds(g, 1), :] = left

    @pl.when(most <= FEW_ROWS)
    def _():
        for g in range(8):
            pack_group(FEW_ROWS, g)

    @pl.when(most > FEW_ROWS)
    def _():
        def pack_next(g, _):
            pack_group(2 * rows, g)
            return 0

        lax.fori_loop(0, 8, pack_next, 0)

    lefts = lefts_ref[...]
    sixteen = lax.broadcasted_iota(jnp.int32, (16, LANES), 0)
    numbers = [(sixteen + 16 * k).astype(jnp.float32).astype(jnp.bfloat16) for k in range(8)]

    def wide(values, s):
        row = jnp.broadcast_to(values[s : s + 1, :].astype(jnp.float32), (16, LANES))
        return row.astype(jnp.bfloat16)

    out_ref[...] = jnp.zeros_like(out_ref)

    def add_blocks(turn, _):
        ats, years, digits, codes, lanes = [], [], [], [], []
        for u in range(4):
            at = pl.ds(pl.multiple_of(turn * 32 + u * 8, 8), 8)
            meta = metas_ref[at, :]
            product = meta & 0xFFFFF
            local = product & 16383
            word = (local * 21846) >> 16
            ats.append(at)
            years.append((meta >> 20) & 15)
            digits.append(local - word * 3)
            codes.append(place_in(product)[1] * 32 + (word >> 7) - c * SPLIT_ROW)
            lanes.append(word & 127)

        def step(part, found):
            found = [list(f) for f in found]
            for q in range(4):
                code = codes[q] - part * 256
                for u in range(8):
                    for i in range(BRAND_ROWS):
                        start = part * (8 * BLOCK_ROWS * 8) + (u * BLOCK_ROWS + i) * 8
                        row = mixed_ref[pl.ds(pl.multiple_of(start, 8), 8), :]
                        got = lane_gather(row, lanes[q])
                        found[q][i % 2] = jnp.where(code == u * 32 + i, got, found[q][i % 2])
            return tuple(tuple(f) for f in found)

        zero = jnp.zeros((8, LANES), jnp.int32)
        found = lax.fori_loop(0, 1, step, ((zero, zero),) * 4)
        weighted, low_hot = [], []
        for u in range(4):
            brand = ((found[u][0] | found[u][1]) >> (digits[u] * 10)) & 1023
            amount = jnp.where(turn * 4 + u < lefts, moneys_ref[ats[u], :], 0.0)
            high = (brand >> 7) * YEARS + years[u]
            low = brand & 127
            one, none = jnp.ones((16, LANES), jnp.bfloat16), jnp.zeros((16, LANES), jnp.bfloat16)
            for s in range(8):
                high_now, low_now, amount_now = (wide(v, s) for v in (high, low, amount))
                weighted.append(
                    jnp.concatenate(
                        [jnp.where(n == high_now, amount_now, none) for n in numbers], axis=0
                    )
                )
                low_hot.append(
                    jnp.concatenate([jnp.where(n == low_now, one, none) for n in numbers], axis=0)
                )
        out_ref[...] += lax.dot_general(
            jnp.concatenate(weighted, axis=1),
            jnp.concatenate(low_hot, axis=1),
            (((1,), (1,)), ((), ())),
            preferred_element_type=jnp.float32,
        )
        return 0

    lax.fori_loop(0, (jnp.max(lefts) + 3) // 4, add_blocks, 0)


def joined(where, own, other, tables):
    vmem = pl.BlockSpec(memory_space=pltpu.VMEM)
    rows = 2 * own[0].shape[0]
    return pl.pallas_call(
        join_kernel,
        out_shape=jax.ShapeDtypeStruct((LANES, LANES), jnp.float32),
        in_specs=[pl.BlockSpec(memory_space=pltpu.SMEM)] + [vmem] * 12,
        out_specs=vmem,
        scratch_shapes=[
            pltpu.VMEM((24, LANES), jnp.int32),
            pltpu.VMEM((rows, LANES), jnp.int32),
            pltpu.VMEM((rows, LANES), jnp.int32),
            pltpu.VMEM((rows, LANES), jnp.float32),
            pltpu.VMEM((8 * rows, LANES), jnp.int32),
            pltpu.VMEM((8 * rows, LANES), jnp.float32),
            pltpu.VMEM((8, LANES), jnp.int32),
            pltpu.VMEM((64 * BLOCK_ROWS, LANES), jnp.int32),
        ],
        cost_estimate=pl.CostEstimate(flops=10**8, bytes_accessed=10**6, transcendentals=0),
        compiler_params=pltpu.CompilerParams(
            vmem_limit_bytes=8 * 2**20
        ),
    )(where, *own, *other, *tables)


def half_kernel(c_ref, packed_ref, out_ref):
    for half in range(2):

        @pl.when(c_ref[0] == half)
        def _(half=half):
            out_ref[:BRAND_ROWS, :] = packed_ref[pl.ds(half * SPLIT_ROW, BRAND_ROWS), :]
            out_ref[BRAND_ROWS:, :] = packed_ref[pl.ds(43 + half * FLAG_ROWS, FLAG_ROWS), :]

    lane = lax.broadcasted_iota(jnp.int32, (1, LANES), 1)
    last = pl.ds(BRAND_ROWS - 1, 1)
    out_ref[last, :] = jnp.where(lane < SMALL_LANE, out_ref[last, :], packed_ref[pl.ds(42, 1), :])


def half_of(c, packed):
    vmem = pl.BlockSpec(memory_space=pltpu.VMEM)
    return pl.pallas_call(
        half_kernel,
        out_shape=jax.ShapeDtypeStruct((BLOCK_ROWS, LANES), jnp.int32),
        in_specs=[pl.BlockSpec(memory_space=pltpu.SMEM), vmem],
        out_specs=vmem,
        compiler_params=pltpu.CompilerParams(vmem_limit_bytes=2**20),
    )(c[None], packed)


def gather_tables(block):
    line = jnp.concatenate(from_behind(block, "z", (1, 2, 3)), axis=0)
    plane = jnp.concatenate(from_behind(line, "y", (1, 3, 2)), axis=0)
    return from_behind(plane, "x", (1, 3, 2))


def four_added(value, axis):
    if axis == "z":
        c, b, a = (swapped(value, axis, bits) for bits in (3, 2, 1))
        return (value + a) + (b + c)
    a, b, c, d = from_behind(value, axis, (1, 3, 2))
    return (a + c) + (b + d)


def sum_everywhere(partial, c):
    def half(at):
        return lax.dynamic_slice_in_dim(partial, at * 64, 64, 0)

    total = half(c) + swapped(half(1 - c), "c", 1)
    for axis in ("x", "y", "z"):
        total = four_added(total, axis)
    total = total + swapped(total, "z", 7)
    return pl.pallas_call(
        lay_kernel,
        out_shape=jax.ShapeDtypeStruct((YEARS, BRANDS), jnp.float32),
        in_specs=[pl.BlockSpec(memory_space=pltpu.SMEM)]
        + [pl.BlockSpec(memory_space=pltpu.VMEM)] * 2,
        out_specs=pl.BlockSpec(memory_space=pltpu.VMEM),
        compiler_params=pltpu.CompilerParams(vmem_limit_bytes=2**20),
    )(c[None], total, swapped(total, "c", 1))


def lay_kernel(c_ref, mine_ref, other_ref, out_ref):
    for side, ref in enumerate((mine_ref, other_ref)):
        for i in range(4):
            at = (c_ref[0] ^ side) * 4 + i
            out_ref[:, pl.ds(pl.multiple_of(at * LANES, LANES), LANES)] = ref[pl.ds(i * 16, 16), :]


def shards(
    date_key,
    store_key,
    product_key,
    revenue,
    row_counts,
    date_years,
    date_flags,
    store_flags,
    product_flags,
    brand_words,
):
    gx, gy = lax.axis_index("gx"), lax.axis_index("gy")
    zl, x, y, c = gx >> 4, (gx >> 2) & 3, gx & 3, gy & 1
    packed = jnp.concatenate(
        [brand_words[: 43 * LANES - 42], store_flags, date_years, date_flags, product_flags]
    ).reshape(47, LANES)
    block = half_of(c, packed)
    live = lax.iota(jnp.int32, product_key.shape[0]) < row_counts[0]
    own = [
        a.reshape(-1, LANES)
        for a in (
            date_key,
            store_key,
            jnp.where(live, product_key, -1),
            revenue.astype(jnp.float32),
        )
    ]
    other = [swapped(a, "c", 1) for a in own]
    tables = gather_tables(block)
    partial = joined(jnp.stack([zl, x, y, c]), own, other, tables)
    return sum_everywhere(partial, c)


def solution(mesh):
    placed = (P(AXES),) * 5 + (P("gx"),) * 5
    return jax.shard_map(shards, mesh=mesh, in_specs=placed, out_specs=P(), check_vma=False)
```
